32 devices in a mesh: model: 4 (over z), data: 8 (over y, x, core).
Axes of the slice: x: 2, y: 2, z: 4, core: 2. Of those that a mesh axis runs over, the one named last changes fastest.
Arguments:
- emb_param: float32 [16384, 1024], P('model', 'data')
- head_param: float32 [1024, 16384], P('data', 'model')
- emb_grad: float32 [8, 16384, 1024], P('data', 'model')
- head_grad: float32 [8, 1024, 16384], P('data', None, 'model')
- emb_row: float32 [16384], P('model')
- emb_col: float32 [1024], P('data')
- head_row: float32 [16384], P('model')
- head_col: float32 [1024], P('data')
Outputs:
- output 1: float32 [16384, 1024], P('model', 'data')
- output 2: float32 [1024, 16384], P('data', 'model')
- output 3: float32 [16384], P('model')
- output 4: float32 [1024], P('data')
- output 5: float32 [16384], P('model')
- output 6: float32 [1024], P('data')
- output 7: bfloat16 [16384, 1024], P('model', 'data')
- output 8: bfloat16 [1024, 16384], P('data', 'model')
All inputs are finite; a program needn't handle non-finite values.
Results may differ from the reference program's by a relative error of at most 0.001.
Values sent between devices are 32-bit elements.
A program may use at most 1 GiB of HBM per device.

```python
import jax
import jax.numpy as jnp

VOCAB_SIZE = 16384
EMBED_DIM = 1024
DATA_REPLICAS = 8
TRAIN_STEP = 10

DECAY_EXP = 0.8
EPS_ONE = 1e-30
CLIP_LIMIT = 1.0
SCALE_FLOOR = 1e-3
LEARN_RATE = float(TRAIN_STEP) ** -0.5
BETA_TWO = 1.0 - float(TRAIN_STEP) ** -DECAY_EXP


def vocab_trend(count):
    position = jnp.arange(count, dtype=jnp.float32) / count
    return 0.4 + 1.2 * (1.0 - position)


def touch_mask(mask_key):
    freq_tier = (8 * jnp.arange(VOCAB_SIZE, dtype=jnp.int32)) // VOCAB_SIZE
    limit = jnp.right_shift(jnp.full((VOCAB_SIZE,), 1024, jnp.int32), freq_tier)
    draws = jax.random.randint(mask_key, (DATA_REPLICAS, VOCAB_SIZE), 0, 1024, dtype=jnp.int32)
    touched = (draws < limit[None, :]).astype(jnp.float32)
    return touched, limit.astype(jnp.float32) / 1024.0


def setup_inputs(seed: int = 0) -> dict:
    rand_keys = jax.random.split(jax.random.key(seed), 16)
    row_trend = vocab_trend(VOCAB_SIZE)
    col_trend = 0.5 + jnp.arange(EMBED_DIM, dtype=jnp.float32) / EMBED_DIM
    rep_scale = DATA_REPLICAS ** -0.5
    emb_param = jax.random.normal(rand_keys[0], (VOCAB_SIZE, EMBED_DIM), jnp.float32) * row_trend[:, None] * col_trend[None, :]
    head_param = 0.5 * jax.random.normal(rand_keys[1], (EMBED_DIM, VOCAB_SIZE), jnp.float32) * col_trend[:, None] * row_trend[None, :]
    emb_rows = jnp.exp(0.5 * jax.random.normal(rand_keys[2], (VOCAB_SIZE,), jnp.float32)) * row_trend
    emb_cols = jnp.exp(0.5 * jax.random.normal(rand_keys[3], (EMBED_DIM,), jnp.float32))
    head_rows = jnp.exp(0.5 * jax.random.normal(rand_keys[4], (VOCAB_SIZE,), jnp.float32)) * row_trend
    head_cols = jnp.exp(0.5 * jax.random.normal(rand_keys[5], (EMBED_DIM,), jnp.float32))
    touched, density = touch_mask(rand_keys[6])
    emb_grad = (jax.random.normal(rand_keys[7], (DATA_REPLICAS, VOCAB_SIZE, EMBED_DIM), jnp.float32)
                * touched[:, :, None] * (rep_scale * emb_rows)[None, :, None] * emb_cols[None, None, :])
    head_grad = (jax.random.normal(rand_keys[8], (DATA_REPLICAS, EMBED_DIM, VOCAB_SIZE), jnp.float32)
                 * (rep_scale * head_cols)[None, :, None] * head_rows[None, None, :])
    emb_row = 0.3 * density * jnp.exp(0.7 * jax.random.normal(rand_keys[9], (VOCAB_SIZE,), jnp.float32))
    emb_col = 0.1 * jnp.exp(0.7 * jax.random.normal(rand_keys[10], (EMBED_DIM,), jnp.float32))
    head_row = 0.3 * jnp.exp(0.7 * jax.random.normal(rand_keys[11], (VOCAB_SIZE,), jnp.float32))
    head_col = 0.3 * jnp.exp(0.7 * jax.random.normal(rand_keys[12], (EMBED_DIM,), jnp.float32))
    return {"emb_param": emb_param, "head_param": head_param, "emb_grad": emb_grad, "head_grad": head_grad,
            "emb_row": emb_row, "emb_col": emb_col, "head_row": head_row, "head_col": head_col}


def adafactor_matrix(param, grad_sum, row_old, col_old, vocab_axis):
    embed_axis = 1 - vocab_axis
    grad_sq = grad_sum * grad_sum + EPS_ONE
    row_new = BETA_TWO * row_old + (1.0 - BETA_TWO) * jnp.mean(grad_sq, axis=embed_axis)
    col_new = BETA_TWO * col_old + (1.0 - BETA_TWO) * jnp.mean(grad_sq, axis=vocab_axis)
    vhat = jnp.expand_dims(row_new, embed_axis) * jnp.expand_dims(col_new, vocab_axis) / jnp.mean(row_new)
    update = grad_sum / jnp.sqrt(vhat)
    update = update / jnp.maximum(1.0, jnp.sqrt(jnp.mean(update * update)) / CLIP_LIMIT)
    step_scale = LEARN_RATE * jnp.maximum(SCALE_FLOOR, jnp.sqrt(jnp.mean(param * param)))
    return param - step_scale * update, row_new, col_new


def reference(emb_param, head_param, emb_grad, head_grad, emb_row, emb_col, head_row, head_col):
    emb_sum = jnp.sum(emb_grad, axis=0)
    head_sum = jnp.sum(head_grad, axis=0)
    emb_new, emb_row_new, emb_col_new = adafactor_matrix(emb_param, emb_sum, emb_row, emb_col, 0)
    head_new, head_row_new, head_col_new = adafactor_matrix(head_param, head_sum, head_row, head_col, 1)
    return (emb_new, head_new, emb_row_new, emb_col_new, head_row_new, head_col_new,
            emb_new.astype(jnp.bfloat16), head_new.astype(jnp.bfloat16))
```

```python
import functools

import jax
import jax.numpy as jnp
from jax import lax
from jax.experimental import pallas as pl
from jax.experimental.pallas import tpu as pltpu
from jax.sharding import PartitionSpec as P

TRAIN_STEP = 10
DECAY_EXP = 0.8
EPS_ONE = 1e-30
CLIP_LIMIT = 1.0
SCALE_FLOOR = 1e-3
LEARN_RATE = float(TRAIN_STEP) ** -0.5
BETA_TWO = 1.0 - float(TRAIN_STEP) ** -DECAY_EXP

MESH = pl.DeviceIdType.MESH
CHUNK = 256
AHEAD = 3
LANES = 128


class Table:
    def __init__(self, grad, out, own, half, first_x, first_y, second_x, second_y, sems, rows):
        self.grad, self.out, self.own, self.half = grad, out, own, half
        self.first_x, self.first_y, self.second_x, self.second_y = first_x, first_y, second_x, second_y
        self.ld, self.ra, self.rfx, self.rfy, self.rgx, self.rgy, self.snd, self.osem = sems
        self.h = rows // 2


def reduce_kernel(steps, emb_grad, head_grad, emb_out, head_out, *scratch):
    emb_buf, head_buf = scratch[:6], scratch[6:12]
    emb_sem, head_sem = scratch[12:20], scratch[20:28]
    emb = Table(emb_grad, emb_out, *emb_buf, emb_sem, CHUNK)
    head = Table(head_grad, head_out, *head_buf, head_sem, LANES)

    z = lax.axis_index("model")
    d = lax.axis_index("data")
    c = lax.rem(d, 2)
    x = lax.rem(d // 2, 2)
    y = d // 4
    partner = (z, d + 1 - 2 * c)
    xnbr = (z, d + 2 - 4 * x)
    ynbr = (z, d + 4 - 8 * y)

    def emb_slice(k, yy, xx, core):
        col = pl.multiple_of(((yy * 2 + xx) * 2 + core) * LANES, LANES)
        return emb_grad.at[pl.ds(pl.multiple_of(k * CHUNK, CHUNK), CHUNK), pl.ds(col, LANES)]

    def head_slice(k, core):
        return head_grad.at[:, :, core, :, pl.ds(pl.multiple_of(k * CHUNK, CHUNK), CHUNK)]

    def load(k, is_emb):
        if is_emb:
            for yy in range(2):
                for xx in range(2):
                    pltpu.make_async_copy(emb_slice(k, yy, xx, c), emb.own.at[k, yy, xx], emb.ld.at[k]).start()
        else:
            pltpu.make_async_copy(head_slice(k, c), head.own.at[k], head.ld.at[k]).start()

    def exchange(k, is_emb):
        if is_emb:
            for yy in range(2):
                for xx in range(2):
                    pltpu.make_async_remote_copy(
                        src_ref=emb_slice(k, yy, xx, 1 - c), dst_ref=emb.half.at[k, yy, xx],
                        send_sem=emb.snd.at[0], recv_sem=emb.ra.at[k],
                        device_id=partner, device_id_type=MESH).start()
        else:
            pltpu.make_async_remote_copy(
                src_ref=head_slice(k, 1 - c), dst_ref=head.half.at[k],
                send_sem=head.snd.at[0], recv_sem=head.ra.at[k],
                device_id=partner, device_id_type=MESH).start()

    def arrived(ref, sem):
        pltpu.make_async_copy(ref, ref, sem).wait()

    def first_hop(k, t):
        arrived(t.own.at[k], t.ld.at[k])
        arrived(t.half.at[k], t.ra.at[k])
        h = t.h
        for yy in range(2):
            t.own[k, yy, 1 - x, :h] += t.half[k, yy, 1 - x, :h]
        pltpu.make_async_remote_copy(
            src_ref=t.own.at[k, :, 1 - x, pl.ds(0, h)], dst_ref=t.first_x.at[k],
            send_sem=t.snd.at[1], recv_sem=t.rfx.at[k], device_id=xnbr, device_id_type=MESH).start()
        for xx in range(2):
            t.own[k, 1 - y, xx, h:] += t.half[k, 1 - y, xx, h:]
        pltpu.make_async_remote_copy(
            src_ref=t.own.at[k, 1 - y, :, pl.ds(h, h)], dst_ref=t.first_y.at[k],
            send_sem=t.snd.at[2], recv_sem=t.rfy.at[k], device_id=ynbr, device_id_type=MESH).start()

    def second_hop(k, t):
        h = t.h
        arrived(t.first_x.at[k], t.rfx.at[k])
        t.own[k, 1 - y, x, :h] += t.half[k, 1 - y, x, :h] + t.first_x[k, 1 - y]
        pltpu.make_async_remote_copy(
            src_ref=t.own.at[k, 1 - y, x, pl.ds(0, h)], dst_ref=t.second_x.at[k],
            send_sem=t.snd.at[3], recv_sem=t.rgx.at[k], device_id=ynbr, device_id_type=MESH).start()
        arrived(t.first_y.at[k], t.rfy.at[k])
        t.own[k, y, 1 - x, h:] += t.half[k, y, 1 - x, h:] + t.first_y[k, 1 - x]
        pltpu.make_async_remote_copy(
            src_ref=t.own.at[k, y, 1 - x, pl.ds(h, h)], dst_ref=t.second_y.at[k],
            send_sem=t.snd.at[4], recv_sem=t.rgy.at[k], device_id=xnbr, device_id_type=MESH).start()

    def finish(k, t, is_emb):
        h = t.h
        arrived(t.second_x.at[k], t.rgx.at[k])
        t.own[k, y, x, :h] += t.half[k, y, x, :h] + t.first_x[k, y] + t.second_x[k]
        arrived(t.second_y.at[k], t.rgy.at[k])
        t.own[k, y, x, h:] += t.half[k, y, x, h:] + t.first_y[k, x] + t.second_y[k]
        span = pl.ds(pl.multiple_of(k * CHUNK, CHUNK), CHUNK)
        dst = t.out.at[span] if is_emb else t.out.at[:, span]
        pltpu.make_async_copy(t.own.at[k, y, x], dst, t.osem.at[0]).start()

    for k in range(AHEAD):
        load(k, True)

    barrier = pltpu.get_barrier_semaphore()
    for peer in (partner, xnbr, ynbr):
        pl.semaphore_signal(barrier, inc=1, device_id=peer, device_id_type=MESH)
    pl.semaphore_wait(barrier, 3)

    for k in range(AHEAD):
        exchange(k, True)

    total = 2 * steps

    def both(k, act):
        @pl.when((k >= 0) & (k < steps))
        def _():
            act(k, emb, True)

        @pl.when((k >= steps) & (k < total))
        def _():
            act(k - steps, head, False)

    def fetch(k, t, is_emb):
        load(k, is_emb)
        exchange(k, is_emb)

    def step(i, carry):
        both(i + AHEAD, fetch)
        both(i, lambda k, t, is_emb: first_hop(k, t))
        both(i - 1, lambda k, t, is_emb: second_hop(k, t))
        both(i - 3, finish)
        return carry

    lax.fori_loop(0, total + 3, step, 0)

    for t in (emb, head):
        arrived(t.half, t.snd.at[0])
        arrived(t.first_x, t.snd.at[1])
        arrived(t.first_y, t.snd.at[2])
        arrived(t.second_x, t.snd.at[3])
        arrived(t.second_y, t.snd.at[4])
        arrived(t.out, t.osem.at[0])


def reduce_tables(emb_grad, head_grad):
    rows, embed = emb_grad.shape
    steps = rows // CHUNK
    head_view = head_grad.reshape(2, 2, 2, LANES, rows)

    def buffers(a, b):
        return [pltpu.VMEM((steps, 2, 2, a, b), jnp.float32), pltpu.VMEM((steps, 2, 2, a, b), jnp.float32),
                pltpu.VMEM((steps, 2, a // 2, b), jnp.float32), pltpu.VMEM((steps, 2, a // 2, b), jnp.float32),
                pltpu.VMEM((steps, a // 2, b), jnp.float32), pltpu.VMEM((steps, a // 2, b), jnp.float32)]

    sems = [pltpu.SemaphoreType.DMA((steps,)) for _ in range(6)]
    sems += [pltpu.SemaphoreType.DMA((5,)), pltpu.SemaphoreType.DMA((1,))]
    return pl.pallas_call(
        functools.partial(reduce_kernel, steps),
        out_shape=(jax.ShapeDtypeStruct((rows, LANES), jnp.float32), jax.ShapeDtypeStruct((LANES, rows), jnp.float32)),
        in_specs=[pl.BlockSpec(memory_space=pl.ANY)] * 2,
        out_specs=[pl.BlockSpec(memory_space=pl.ANY)] * 2,
        scratch_shapes=buffers(CHUNK, LANES) + buffers(LANES, CHUNK) + sems + sems,
        compiler_params=pltpu.CompilerParams(collective_id=0, has_side_effects=True, vmem_limit_bytes=60 * 1024 * 1024),
    )(emb_grad, head_view)


def apply_step(param, grad_sum, row_old, col_old, row_sq, col_sq, vocab_axis, vocab, embed):
    embed_axis = 1 - vocab_axis
    row_new = BETA_TWO * row_old + (1.0 - BETA_TWO) * (row_sq / embed)
    col_new = BETA_TWO * col_old + (1.0 - BETA_TWO) * (col_sq / vocab)
    row_mean = lax.psum(jnp.sum(row_new), "model") / vocab
    row_factor = jnp.expand_dims(lax.rsqrt(row_new), embed_axis)
    col_factor = jnp.expand_dims(lax.rsqrt(col_new) * jnp.sqrt(row_mean), vocab_axis)
    update = grad_sum * row_factor * col_factor
    update_rms = jnp.sqrt(lax.psum(jnp.sum(update * update), ("model", "data")) / (vocab * embed))
    param_rms = jnp.sqrt(lax.psum(jnp.sum(param * param), ("model", "data")) / (vocab * embed))
    step_size = LEARN_RATE * jnp.maximum(SCALE_FLOOR, param_rms) / jnp.maximum(1.0, update_rms / CLIP_LIMIT)
    return param - step_size * update, row_new, col_new


def block_update(param, grad_sum, row_old, col_old, vocab_axis, vocab, embed):
    embed_axis = 1 - vocab_axis
    grad_sq = grad_sum * grad_sum + EPS_ONE
    row_sq = lax.psum(jnp.sum(grad_sq, axis=embed_axis), "data")
    col_sq = lax.psum(jnp.sum(grad_sq, axis=vocab_axis), "model")
    return apply_step(param, grad_sum, row_old, col_old, row_sq, col_sq, vocab_axis, vocab, embed)


def solution(mesh):
    arg_specs = (P("model", "data"), P("data", "model"), P("data", "model", None), P("data", None, "model"),
                 P("model"), P("data"), P("model"), P("data"))
    result_specs = (P("model", "data"), P("data", "model"), P("model"), P("data"), P("model"), P("data"),
                    P("model", "data"), P("data", "model"))

    def update_tables(emb_param, head_param, emb_grad, head_grad, emb_row, emb_col, head_row, head_col):
        vocab = emb_param.shape[0]
        embed = emb_param.shape[1]

        def local_step(emb_block, head_block, emb_contrib, head_contrib, emb_rows, emb_cols, head_rows, head_cols):
            emb_sum, head_sum = reduce_tables(emb_contrib[0], head_contrib[0])
            emb_new, emb_row_new, emb_col_new = block_update(emb_block, emb_sum, emb_rows, emb_cols, 0, vocab, embed)
            head_new, head_row_new, head_col_new = block_update(head_block, head_sum, head_rows, head_cols, 1, vocab, embed)
            return (emb_new, head_new, emb_row_new, emb_col_new, head_row_new, head_col_new,
                    emb_new.astype(jnp.bfloat16), head_new.astype(jnp.bfloat16))

        mapped = jax.shard_map(local_step, mesh=mesh, in_specs=arg_specs, out_specs=result_specs, check_vma=False)
        return mapped(emb_param, head_param, emb_grad, head_grad, emb_row, emb_col, head_row, head_col)

    return update_tables
```

```python
import functools

import jax
import jax.numpy as jnp
from jax import lax
from jax.experimental import pallas as pl
from jax.experimental.pallas import tpu as pltpu
from jax.sharding import PartitionSpec as P

TRAIN_STEP = 10
DECAY_EXP = 0.8
EPS_ONE = 1e-30
CLIP_LIMIT = 1.0
SCALE_FLOOR = 1e-3
LEARN_RATE = float(TRAIN_STEP) ** -0.5
BETA_TWO = 1.0 - float(TRAIN_STEP) ** -DECAY_EXP

MESH = pl.DeviceIdType.MESH
CHUNK = 256
AHEAD = 3
LANES = 128
VMEM_MIB = 54


class Table:
    def __init__(self, is_emb, grad, param, row, col, outs, bufs, small, sems):
        self.is_emb, self.grad, self.param, self.row, self.col = is_emb, grad, param, row, col
        self.dirn, self.pcopy, self.row_new, self.col_new, self.scale = outs
        self.own, self.half, self.first_x, self.first_y, self.second_x, self.second_y = bufs
        self.rpart, self.rrecv, self.col_acc, self.w_acc, self.r_acc, self.p_acc, self.colx, self.scalx, self.vec = small
        (self.ld, self.ra, self.rfx, self.rfy, self.rgx, self.rgy, self.rr0, self.rr1, self.rr2, self.snd, self.one) = sems
        self.rr = (self.rr0, self.rr1, self.rr2)
        self.h = (CHUNK if is_emb else LANES) // 2


N_OUT, N_BUF, N_SMALL, N_SEM = 5, 6, 9, 11


def arrived(ref, sem):
    pltpu.make_async_copy(ref, ref, sem).wait()


def lane_sum(a):
    return jnp.sum(a, axis=1, keepdims=True)


def fold8(a):
    return jnp.sum(a.reshape(a.shape[0] // 8, 8, a.shape[1]), axis=0)


def adafactor_kernel(steps, nz, nd, *refs):
    emb_in, head_in = refs[0:4], refs[4:8]
    pos = 8
    emb_out, head_out = refs[pos:pos + N_OUT], refs[pos + N_OUT:pos + 2 * N_OUT]
    pos += 2 * N_OUT
    emb_buf, head_buf = refs[pos:pos + N_BUF], refs[pos + N_BUF:pos + 2 * N_BUF]
    pos += 2 * N_BUF
    emb_small, head_small = refs[pos:pos + N_SMALL], refs[pos + N_SMALL:pos + 2 * N_SMALL]
    pos += 2 * N_SMALL
    emb_sem, head_sem = refs[pos:pos + N_SEM], refs[pos + N_SEM:pos + 2 * N_SEM]
    emb = Table(True, *emb_in, emb_out, emb_buf, emb_small, emb_sem)
    head = Table(False, *head_in, head_out, head_buf, head_small, head_sem)
    vocab, embed = float(nz * steps * CHUNK), float(nd * LANES)
    others = nz * nd - 1

    z = lax.axis_index("model")
    d = lax.axis_index("data")
    me = z * nd + d
    c = lax.rem(d, 2)
    x = lax.rem(d // 2, 2)
    y = d // 4
    partner = (z, d + 1 - 2 * c)
    xnbr = (z, d + 2 - 4 * x)
    ynbr = (z, d + 4 - 8 * y)
    ring = (partner, xnbr, ynbr)

    def emb_slice(k, yy, xx, core):
        col = pl.multiple_of(((yy * 2 + xx) * 2 + core) * LANES, LANES)
        return emb.grad.at[pl.ds(pl.multiple_of(k * CHUNK, CHUNK), CHUNK), pl.ds(col, LANES)]

    def head_slice(k, core):
        return head.grad.at[:, :, core, :, pl.ds(pl.multiple_of(k * CHUNK, CHUNK), CHUNK)]

    def send(src, dst, ssem, rsem, to):
        pltpu.make_async_remote_copy(src_ref=src, dst_ref=dst, send_sem=ssem, recv_sem=rsem,
                                     device_id=to, device_id_type=MESH).start()

    def load(k, t):
        if t.is_emb:
            for yy in range(2):
                for xx in range(2):
                    pltpu.make_async_copy(emb_slice(k, yy, xx, c), t.own.at[k, yy, xx], t.ld.at[k]).start()
        else:
            pltpu.make_async_copy(head_slice(k, c), t.own.at[k], t.ld.at[k]).start()

    def exchange(k, t):
        if t.is_emb:
            for yy in range(2):
                for xx in range(2):
                    send(emb_slice(k, yy, xx, 1 - c), t.half.at[k, yy, xx], t.snd.at[0], t.ra.at[k], partner)
        else:
            send(head_slice(k, 1 - c), t.half.at[k], t.snd.at[0], t.ra.at[k], partner)

    def first_hop(k, t):
        arrived(t.own.at[k], t.ld.at[k])
        arrived(t.half.at[k], t.ra.at[k])
        h = t.h
        for yy in range(2):
            t.own[k, yy, 1 - x, :h] += t.half[k, yy, 1 - x, :h]
        send(t.own.at[k, :, 1 - x, pl.ds(0, h)], t.first_x.at[k], t.snd.at[1], t.rfx.at[k], xnbr)
        for xx in range(2):
            t.own[k, 1 - y, xx, h:] += t.half[k, 1 - y, xx, h:]
        send(t.own.at[k, 1 - y, :, pl.ds(h, h)], t.first_y.at[k], t.snd.at[2], t.rfy.at[k], ynbr)

    def second_hop(k, t):
        h = t.h
        arrived(t.first_x.at[k], t.rfx.at[k])
        t.own[k, 1 - y, x, :h] += t.half[k, 1 - y, x, :h] + t.first_x[k, 1 - y]
        send(t.own.at[k, 1 - y, x, pl.ds(0, h)], t.second_x.at[k], t.snd.at[3], t.rgx.at[k], ynbr)
        arrived(t.first_y.at[k], t.rfy.at[k])
        t.own[k, y, 1 - x, h:] += t.half[k, y, 1 - x, h:] + t.first_y[k, 1 - x]
        send(t.own.at[k, y, 1 - x, pl.ds(h, h)], t.second_y.at[k], t.snd.at[4], t.rgy.at[k], xnbr)

    def tile(k, i):
        return pl.ds(pl.multiple_of(k * CHUNK + i * LANES, LANES), LANES)

    def finish(k, t):
        h = t.h
        arrived(t.second_x.at[k], t.rgx.at[k])
        arrived(t.second_y.at[k], t.rgy.at[k])
        first = t.own[k, y, x, :h] + t.half[k, y, x, :h] + t.first_x[k, y] + t.second_x[k]
        last = t.own[k, y, x, h:] + t.half[k, y, x, h:] + t.first_y[k, x] + t.second_y[k]
        if t.is_emb:
            for i, g in enumerate((first, last)):
                t.dirn[tile(k, i), :] = g
                sq = g * g + EPS_ONE
                t.col_acc[...] += fold8(sq)
                t.rpart[0, k, i:i + 1, :] = jnp.sum(jnp.transpose(sq), axis=0, keepdims=True)
                p = t.pcopy[tile(k, i), :]
                t.p_acc[...] += fold8(p * p)
        else:
            for i in range(CHUNK // LANES):
                lanes = slice(i * LANES, (i + 1) * LANES)
                t.dirn[:h, tile(k, i)] = first[:, lanes]
                t.dirn[h:, tile(k, i)] = last[:, lanes]
                sq_first = first[:, lanes] * first[:, lanes] + EPS_ONE
                sq_last = last[:, lanes] * last[:, lanes] + EPS_ONE
                t.col_acc[:h] += sq_first
                t.col_acc[h:] += sq_last
                t.rpart[0, k, i:i + 1, :] = jnp.sum(fold8(sq_first) + fold8(sq_last), axis=0, keepdims=True)
                p = t.pcopy[:, tile(k, i)]
                t.p_acc[...] += fold8(p * p)
        send(t.rpart.at[0, k], t.rrecv.at[0, k], t.snd.at[5], t.rr[0].at[k], ring[0])

    def row_hop(s, k, t):
        arrived(t.rrecv.at[s - 1, k], t.rr[s - 1].at[k])
        t.rpart[s, k] = t.rpart[s - 1, k] + t.rrecv[s - 1, k]
        send(t.rpart.at[s, k], t.rrecv.at[s, k], t.snd.at[5 + s], t.rr[s].at[k], ring[s])

    def complete(k, t):
        arrived(t.rrecv.at[2, k], t.rr[2].at[k])
        row_sq = t.rpart[2, k] + t.rrecv[2, k]
        rows = pl.ds(k * (CHUNK // LANES), CHUNK // LANES)
        new = BETA_TWO * t.row[rows, :] + (1.0 - BETA_TWO) * (row_sq / embed)
        t.row_new[rows, :] = new
        t.r_acc[...] += new
        factor = lax.rsqrt(new)
        for i in range(CHUNK // LANES):
            line = jnp.broadcast_to(factor[i:i + 1, :], (LANES, LANES))
            if t.is_emb:
                n = t.dirn[tile(k, i), :] * jnp.transpose(line)
                t.dirn[tile(k, i), :] = n
                t.w_acc[...] += fold8(n * n)
            else:
                n = t.dirn[:, tile(k, i)] * line
                t.dirn[:, tile(k, i)] = n
                t.w_acc[...] += n * n

    def per_col(t, acc):
        a = acc[...]
        return jnp.sum(a if t.is_emb else jnp.transpose(a), axis=0, keepdims=True)

    def send_cols(t):
        t.vec[0] = per_col(t, t.col_acc)
        for o in range(1, nz):
            send(t.vec.at[0], t.colx.at[z], t.one.at[0], t.one.at[1], (lax.rem(z + o, nz), d))

    def send_scalars(t):
        arrived(t.colx.at[pl.ds(0, nz - 1)], t.one.at[1])
        t.colx[z] = t.vec[0]
        col_sq = t.colx[0]
        for i in range(1, nz):
            col_sq = col_sq + t.colx[i]
        new = BETA_TWO * t.col[...] + (1.0 - BETA_TWO) * (col_sq / vocab)
        t.col_new[...] = new
        w = lane_sum(per_col(t, t.w_acc) / new)
        r = lane_sum(jnp.sum(t.r_acc[...], axis=0, keepdims=True)) / nd
        p = lane_sum(jnp.sum(t.p_acc[...], axis=0, keepdims=True))
        lane = lax.broadcasted_iota(jnp.int32, (1, LANES), 1)
        t.vec[1] = jnp.where(lane == 0, w, jnp.where(lane == 1, r, jnp.where(lane == 2, p, 0.0)))

        def one(o, carry):
            to = lax.rem(me + o, others + 1)
            send(t.vec.at[1], t.scalx.at[me], t.one.at[2], t.one.at[3], (to // nd, lax.rem(to, nd)))
            return carry

        lax.fori_loop(1, others + 1, one, 0)

    def finish_scalars(t):
        arrived(t.scalx.at[pl.ds(0, others)], t.one.at[3])
        t.scalx[me] = t.vec[1]
        total = jnp.sum(t.scalx[...], axis=0)
        lane = lax.broadcasted_iota(jnp.int32, (1, LANES), 1)
        w, r, p = (lane_sum(jnp.where(lane == i, total, 0.0)) for i in range(3))
        row_mean = r / vocab
        update_rms = jnp.sqrt(w * row_mean / (vocab * embed))
        param_rms = jnp.sqrt(p / (vocab * embed))
        step_size = LEARN_RATE * jnp.maximum(SCALE_FLOOR, param_rms) / jnp.maximum(1.0, update_rms / CLIP_LIMIT)
        line = lax.rsqrt(t.col_new[...]) * (jnp.sqrt(row_mean) * step_size)
        if t.is_emb:
            t.scale[...] = jnp.broadcast_to(line, t.scale.shape)
        else:
            t.scale[...] = jnp.transpose(jnp.broadcast_to(line, (LANES, LANES)))

    for k in range(AHEAD):
        load(k, emb)
    for t in (emb, head):
        pltpu.make_async_copy(t.param, t.pcopy, t.one.at[4]).start()
        for acc in (t.col_acc, t.w_acc, t.r_acc, t.p_acc):
            acc[...] = jnp.zeros_like(acc)

    barrier = pltpu.get_barrier_semaphore()

    def greet(o, carry):
        to = lax.rem(me + o, others + 1)
        pl.semaphore_signal(barrier, inc=1, device_id=(to // nd, lax.rem(to, nd)), device_id_type=MESH)
        return carry

    lax.fori_loop(1, others + 1, greet, 0)
    pl.semaphore_wait(barrier, others)

    for k in range(AHEAD):
        exchange(k, emb)
    for t in (emb, head):
        arrived(t.pcopy, t.one.at[4])

    total = 2 * steps

    def both(k, act):
        @pl.when((k >= 0) & (k < steps))
        def _():
            act(k, emb)

        @pl.when((k >= steps) & (k < total))
        def _():
            act(k - steps, head)

    def fetch(k, t):
        load(k, t)
        exchange(k, t)

    def step(i, carry):
        both(i + AHEAD, fetch)
        both(i, first_hop)
        both(i - 1, second_hop)
        both(i - 3, finish)

        @pl.when(i == steps + 2)
        def _():
            send_cols(emb)

        @pl.when(i == total + 2)
        def _():
            send_cols(head)

        both(i - 4, functools.partial(row_hop, 1))
        both(i - 6, functools.partial(row_hop, 2))
        both(i - 8, complete)

        @pl.when(i == steps + 8)
        def _():
            send_scalars(emb)

        @pl.when(i == steps + 11)
        def _():
            finish_scalars(emb)

        return carry

    lax.fori_loop(0, total + 8, step, 0)
    send_scalars(head)
    finish_scalars(head)

    for t in (emb, head):
        arrived(t.half, t.snd.at[0])
        arrived(t.first_x, t.snd.at[1])
        arrived(t.first_y, t.snd.at[2])
        arrived(t.second_x, t.snd.at[3])
        arrived(t.second_y, t.snd.at[4])
        for s in range(3):
            arrived(t.rpart.at[s], t.snd.at[5 + s])
        arrived(t.colx.at[pl.ds(0, nz - 1)], t.one.at[0])
        arrived(t.scalx.at[pl.ds(0, others)], t.one.at[2])


def statistics(mesh, emb_grad, head_grad, emb_param, head_param, emb_row, emb_col, head_row, head_col):
    rows = emb_grad.shape[0]
    steps = rows // CHUNK
    nz, nd = mesh.shape["model"], mesh.shape["data"]
    f32 = jnp.float32

    def buffers(a, b):
        return [pltpu.VMEM((steps, 2, 2, a, b), f32), pltpu.VMEM((steps, 2, 2, a, b), f32),
                pltpu.VMEM((steps, 2, a // 2, b), f32), pltpu.VMEM((steps, 2, a // 2, b), f32),
                pltpu.VMEM((steps, a // 2, b), f32), pltpu.VMEM((steps, a // 2, b), f32)]

    def small(acc_rows):
        per = CHUNK // LANES
        return [pltpu.VMEM((3, steps, per, LANES), f32), pltpu.VMEM((3, steps, per, LANES), f32),
                pltpu.VMEM((acc_rows, LANES), f32), pltpu.VMEM((acc_rows, LANES), f32),
                pltpu.VMEM((per, LANES), f32), pltpu.VMEM((8, LANES), f32),
                pltpu.VMEM((nz, 1, LANES), f32), pltpu.VMEM((nz * nd, 1, LANES), f32), pltpu.VMEM((2, 1, LANES), f32)]

    sems = [pltpu.SemaphoreType.DMA((steps,)) for _ in range(9)]
    sems += [pltpu.SemaphoreType.DMA((8,)), pltpu.SemaphoreType.DMA((5,))]

    def outs(shape, scale_rows):
        return [jax.ShapeDtypeStruct(shape, f32), jax.ShapeDtypeStruct(shape, f32),
                jax.ShapeDtypeStruct((rows // LANES, LANES), f32), jax.ShapeDtypeStruct((1, LANES), f32),
                jax.ShapeDtypeStruct((scale_rows, LANES), f32)]

    anyspace = pl.BlockSpec(memory_space=pl.ANY)
    vmem = pl.BlockSpec(memory_space=pltpu.VMEM)
    results = pl.pallas_call(
        functools.partial(adafactor_kernel, steps, nz, nd),
        out_shape=outs((rows, LANES), 8) + outs((LANES, rows), LANES),
        in_specs=[anyspace, anyspace, vmem, vmem] * 2,
        out_specs=[vmem] * 10,
        scratch_shapes=(buffers(CHUNK, LANES) + buffers(LANES, CHUNK) + small(8) + small(LANES) + sems + sems),
        compiler_params=pltpu.CompilerParams(collective_id=0, has_side_effects=True, vmem_limit_bytes=VMEM_MIB * 2 ** 20),
    )(emb_grad, emb_param, emb_row.reshape(rows // LANES, LANES), emb_col.reshape(1, LANES),
      head_grad.reshape(2, 2, 2, LANES, rows), head_param, head_row.reshape(rows // LANES, LANES),
      head_col.reshape(1, LANES))
    return results[:5], results[5:]


PIECES = 8


def apply_kernel(rows, *refs):
    (emb_dir, emb_p, emb_r, emb_c, emb_s, head_dir, head_p, head_r, head_c, head_s,
     emb_new, emb_b16, head_new, head_b16, emb_ro, emb_co, head_ro, head_co,
     emb_tmp, emb_tmp16, head_tmp, head_tmp16, sem) = refs
    size = rows // PIECES

    def piece(j, carry):
        span = pl.ds(pl.multiple_of(j * size, size), size)
        new = emb_p[span, :] - emb_dir[span, :] * emb_s[0:1, :]
        emb_tmp[span, :] = new
        emb_tmp16[span, :] = new.astype(jnp.bfloat16)
        pltpu.make_async_copy(emb_tmp.at[span], emb_new.at[span], sem.at[0]).start()
        pltpu.make_async_copy(emb_tmp16.at[span], emb_b16.at[span], sem.at[1]).start()
        for i in range(size // LANES):
            cols = pl.ds(pl.multiple_of(j * size + i * LANES, LANES), LANES)
            new = head_p[:, cols] - head_dir[:, cols] * head_s[...]
            head_tmp[:, cols] = new
            head_tmp16[:, cols] = new.astype(jnp.bfloat16)
        pltpu.make_async_copy(head_tmp.at[:, span], head_new.at[:, span], sem.at[2]).start()
        pltpu.make_async_copy(head_tmp16.at[:, span], head_b16.at[:, span], sem.at[3]).start()
        return carry

    emb_ro[...] = emb_r[...]
    emb_co[...] = emb_c[...]
    head_ro[...] = head_r[...]
    head_co[...] = head_c[...]
    lax.fori_loop(0, PIECES, piece, 0)
    arrived(emb_new, sem.at[0])
    arrived(emb_b16, sem.at[1])
    arrived(head_new, sem.at[2])
    arrived(head_b16, sem.at[3])


def apply_update(emb, head):
    rows = emb[0].shape[0]
    f32, b16 = jnp.float32, jnp.bfloat16
    anyspace = pl.BlockSpec(memory_space=pl.ANY)
    vmem = pl.BlockSpec(memory_space=pltpu.VMEM)
    shapes = ((rows, LANES), f32), ((rows, LANES), b16), ((LANES, rows), f32), ((LANES, rows), b16)
    small = ((rows // LANES, LANES), f32), ((1, LANES), f32)
    emb_new, emb_b16, head_new, head_b16, emb_r, emb_c, head_r, head_c = pl.pallas_call(
        functools.partial(apply_kernel, rows),
        out_shape=[jax.ShapeDtypeStruct(s, t) for s, t in shapes + small + small],
        in_specs=[vmem] * 10,
        out_specs=[anyspace] * 4 + [vmem] * 4,
        scratch_shapes=[pltpu.VMEM(s, t) for s, t in shapes] + [pltpu.SemaphoreType.DMA((4,))],
        compiler_params=pltpu.CompilerParams(vmem_limit_bytes=24 * 2 ** 20),
    )(*emb, *head)
    return (emb_new, head_new, emb_r.reshape(rows), emb_c.reshape(LANES), head_r.reshape(rows), head_c.reshape(LANES),
            emb_b16, head_b16)


def solution(mesh):
    arg_specs = (P("model", "data"), P("data", "model"), P("data", "model", None), P("data", None, "model"),
                 P("model"), P("data"), P("model"), P("data"))
    result_specs = (P("model", "data"), P("data", "model"), P("model"), P("data"), P("model"), P("data"),
                    P("model", "data"), P("data", "model"))

    def local_step(emb_block, head_block, emb_contrib, head_contrib, emb_rows, emb_cols, head_rows, head_cols):
        emb, head = statistics(mesh, emb_contrib[0], head_contrib[0], emb_block, head_block,
                               emb_rows, emb_cols, head_rows, head_cols)
        return apply_update(emb, head)

    return jax.shard_map(local_step, mesh=mesh, in_specs=arg_specs, out_specs=result_specs, check_vma=False)
```

```python
import functools

import jax
import jax.numpy as jnp
from jax import lax
from jax.experimental import pallas as pl
from jax.experimental.pallas import tpu as pltpu
from jax.sharding import PartitionSpec as P

TRAIN_STEP = 10
DECAY_EXP = 0.8
EPS_ONE = 1e-30
CLIP_LIMIT = 1.0
SCALE_FLOOR = 1e-3
LEARN_RATE = float(TRAIN_STEP) ** -0.5
BETA_TWO = 1.0 - float(TRAIN_STEP) ** -DECAY_EXP

MESH = pl.DeviceIdType.MESH
CHUNK = 256
AHEAD = 3
LANES = 128
VMEM_MIB = 45


class Table:
    def __init__(self, is_emb, grad, param, row_old, col_old, outs, bufs, small, sems):
        self.is_emb, self.grad, self.param, self.row_old, self.col_old = is_emb, grad, param, row_old, col_old
        self.dirn, self.pcopy, self.row_new, self.col_new, self.scale = outs
        self.own, self.half, self.first_x, self.first_y, self.second_x, self.second_y = bufs
        self.rpart, self.rrecv, self.col_acc, self.w_acc, self.r_acc, self.p_acc, self.colx, self.scalx, self.vec, self.row, self.col = small
        (self.ld, self.ra, self.rfx, self.rfy, self.rgx, self.rgy, self.rr0, self.rr1, self.rr2, self.snd, self.one) = sems
        self.rr = (self.rr0, self.rr1, self.rr2)
        self.h = (CHUNK if is_emb else LANES) // 2


N_OUT, N_BUF, N_SMALL, N_SEM = 5, 6, 11, 11


def arrived(ref, sem):
    pltpu.make_async_copy(ref, ref, sem).wait()


def lane_sum(a):
    return jnp.sum(a, axis=1, keepdims=True)


def fold8(a):
    return jnp.sum(a.reshape(a.shape[0] // 8, 8, a.shape[1]), axis=0)


def adafactor_kernel(steps, nz, nd, *refs):
    emb_in, head_in = refs[0:4], refs[4:8]
    pos = 8
    emb_out, head_out = refs[pos:pos + N_OUT], refs[pos + N_OUT:pos + 2 * N_OUT]
    pos += 2 * N_OUT
    emb_buf, head_buf = refs[pos:pos + N_BUF], refs[pos + N_BUF:pos + 2 * N_BUF]
    pos += 2 * N_BUF
    emb_small, head_small = refs[pos:pos + N_SMALL], refs[pos + N_SMALL:pos + 2 * N_SMALL]
    pos += 2 * N_SMALL
    emb_sem, head_sem = refs[pos:pos + N_SEM], refs[pos + N_SEM:pos + 2 * N_SEM]
    emb = Table(True, *emb_in, emb_out, emb_buf, emb_small, emb_sem)
    head = Table(False, *head_in, head_out, head_buf, head_small, head_sem)
    vocab, embed = float(nz * steps * CHUNK), float(nd * LANES)
    others = nz * nd - 1

    z = lax.axis_index("model")
    d = lax.axis_index("data")
    me = z * nd + d
    c = lax.rem(d, 2)
    x = lax.rem(d // 2, 2)
    y = d // 4
    partner = (z, d + 1 - 2 * c)
    xnbr = (z, d + 2 - 4 * x)
    ynbr = (z, d + 4 - 8 * y)
    ring = (partner, xnbr, ynbr)

    def emb_slice(k, yy, xx, core):
        col = pl.multiple_of(((yy * 2 + xx) * 2 + core) * LANES, LANES)
        return emb.grad.at[pl.ds(pl.multiple_of(k * CHUNK, CHUNK), CHUNK), pl.ds(col, LANES)]

    def head_slice(k, core):
        return head.grad.at[:, :, core, :, pl.ds(pl.multiple_of(k * CHUNK, CHUNK), CHUNK)]

    def send(src, dst, ssem, rsem, to):
        pltpu.make_async_remote_copy(src_ref=src, dst_ref=dst, send_sem=ssem, recv_sem=rsem,
                                     device_id=to, device_id_type=MESH).start()

    def load(k, t):
        if t.is_emb:
            for yy in range(2):
                for xx in range(2):
                    pltpu.make_async_copy(emb_slice(k, yy, xx, c), t.own.at[k, yy, xx], t.ld.at[k]).start()
        else:
            pltpu.make_async_copy(head_slice(k, c), t.own.at[k], t.ld.at[k]).start()

    def exchange(k, t):
        if t.is_emb:
            for yy in range(2):
                for xx in range(2):
                    send(emb_slice(k, yy, xx, 1 - c), t.half.at[k, yy, xx], t.snd.at[0], t.ra.at[k], partner)
        else:
            send(head_slice(k, 1 - c), t.half.at[k], t.snd.at[0], t.ra.at[k], partner)

    def first_hop(k, t):
        arrived(t.own.at[k], t.ld.at[k])
        arrived(t.half.at[k], t.ra.at[k])
        h = t.h
        for yy in range(2):
            t.own[k, yy, 1 - x, :h] += t.half[k, yy, 1 - x, :h]
        send(t.own.at[k, :, 1 - x, pl.ds(0, h)], t.first_x.at[k], t.snd.at[1], t.rfx.at[k], xnbr)
        for xx in range(2):
            t.own[k, 1 - y, xx, h:] += t.half[k, 1 - y, xx, h:]
        send(t.own.at[k, 1 - y, :, pl.ds(h, h)], t.first_y.at[k], t.snd.at[2], t.rfy.at[k], ynbr)

    def second_hop(k, t):
        h = t.h
        arrived(t.first_x.at[k], t.rfx.at[k])
        t.own[k, 1 - y, x, :h] += t.half[k, 1 - y, x, :h] + t.first_x[k, 1 - y]
        send(t.own.at[k, 1 - y, x, pl.ds(0, h)], t.second_x.at[k], t.snd.at[3], t.rgx.at[k], ynbr)
        arrived(t.first_y.at[k], t.rfy.at[k])
        t.own[k, y, 1 - x, h:] += t.half[k, y, 1 - x, h:] + t.first_y[k, 1 - x]
        send(t.own.at[k, y, 1 - x, pl.ds(h, h)], t.second_y.at[k], t.snd.at[4], t.rgy.at[k], xnbr)

    def tile(k, i):
        return pl.ds(pl.multiple_of(k * CHUNK + i * LANES, LANES), LANES)

    def finish(k, t):
        h = t.h
        arrived(t.second_x.at[k], t.rgx.at[k])
        arrived(t.second_y.at[k], t.rgy.at[k])
        first = t.own[k, y, x, :h] + t.half[k, y, x, :h] + t.first_x[k, y] + t.second_x[k]
        last = t.own[k, y, x, h:] + t.half[k, y, x, h:] + t.first_y[k, x] + t.second_y[k]
        if t.is_emb:
            for i, g in enumerate((first, last)):
                t.dirn[tile(k, i), :] = g
                sq = g * g + EPS_ONE
                t.col_acc[...] += fold8(sq)
                t.rpart[0, k, i:i + 1, :] = jnp.sum(jnp.transpose(sq), axis=0, keepdims=True)
                p = t.pcopy[tile(k, i), :]
                t.p_acc[...] += fold8(p * p)
        else:
            for i in range(CHUNK // LANES):
                lanes = slice(i * LANES, (i + 1) * LANES)
                t.dirn[:h, tile(k, i)] = first[:, lanes]
                t.dirn[h:, tile(k, i)] = last[:, lanes]
                sq_first = first[:, lanes] * first[:, lanes] + EPS_ONE
                sq_last = last[:, lanes] * last[:, lanes] + EPS_ONE
                t.col_acc[:h] += sq_first
                t.col_acc[h:] += sq_last
                t.rpart[0, k, i:i + 1, :] = jnp.sum(fold8(sq_first) + fold8(sq_last), axis=0, keepdims=True)
                p = t.pcopy[:, tile(k, i)]
                t.p_acc[...] += fold8(p * p)
        send(t.rpart.at[0, k], t.rrecv.at[0, k], t.snd.at[5], t.rr[0].at[k], ring[0])

    def row_hop(s, k, t):
        arrived(t.rrecv.at[s - 1, k], t.rr[s - 1].at[k])
        t.rpart[s, k] = t.rpart[s - 1, k] + t.rrecv[s - 1, k]
        send(t.rpart.at[s, k], t.rrecv.at[s, k], t.snd.at[5 + s], t.rr[s].at[k], ring[s])

    def complete(k, t):
        arrived(t.rrecv.at[2, k], t.rr[2].at[k])
        row_sq = t.rpart[2, k] + t.rrecv[2, k]
        rows = pl.ds(k * (CHUNK // LANES), CHUNK // LANES)
        new = BETA_TWO * t.row[rows, :] + (1.0 - BETA_TWO) * (row_sq / embed)
        t.row_new[rows, :] = new
        t.r_acc[...] += new
        factor = lax.rsqrt(new)
        for i in range(CHUNK // LANES):
            line = jnp.broadcast_to(factor[i:i + 1, :], (LANES, LANES))
            if t.is_emb:
                n = t.dirn[tile(k, i), :] * jnp.transpose(line)
                t.dirn[tile(k, i), :] = n
                t.w_acc[...] += fold8(n * n)
            else:
                n = t.dirn[:, tile(k, i)] * line
                t.dirn[:, tile(k, i)] = n
                t.w_acc[...] += n * n

    def per_col(t, acc):
        a = acc[...]
        return jnp.sum(a if t.is_emb else jnp.transpose(a), axis=0, keepdims=True)

    def send_cols(t):
        t.vec[0] = per_col(t, t.col_acc)
        for o in range(1, nz):
            send(t.vec.at[0], t.colx.at[z], t.one.at[0], t.one.at[1], (lax.rem(z + o, nz), d))

    def send_scalars(t):
        arrived(t.colx.at[pl.ds(0, nz - 1)], t.one.at[1])
        t.colx[z] = t.vec[0]
        col_sq = t.colx[0]
        for i in range(1, nz):
            col_sq = col_sq + t.colx[i]
        new = BETA_TWO * t.col[...] + (1.0 - BETA_TWO) * (col_sq / vocab)
        t.col_new[...] = new
        w = lane_sum(per_col(t, t.w_acc) / new)
        r = lane_sum(jnp.sum(t.r_acc[...], axis=0, keepdims=True)) / nd
        p = lane_sum(jnp.sum(t.p_acc[...], axis=0, keepdims=True))
        lane = lax.broadcasted_iota(jnp.int32, (1, LANES), 1)
        t.vec[1] = jnp.where(lane == 0, w, jnp.where(lane == 1, r, jnp.where(lane == 2, p, 0.0)))

        def one(o, carry):
            to = lax.rem(me + o, others + 1)
            send(t.vec.at[1], t.scalx.at[me], t.one.at[2], t.one.at[3], (to // nd, lax.rem(to, nd)))
            return carry

        lax.fori_loop(1, others + 1, one, 0)

    def finish_scalars(t):
        arrived(t.scalx.at[pl.ds(0, others)], t.one.at[3])
        t.scalx[me] = t.vec[1]
        total = jnp.sum(t.scalx[...], axis=0)
        lane = lax.broadcasted_iota(jnp.int32, (1, LANES), 1)
        w, r, p = (lane_sum(jnp.where(lane == i, total, 0.0)) for i in range(3))
        row_mean = r / vocab
        update_rms = jnp.sqrt(w * row_mean / (vocab * embed))
        param_rms = jnp.sqrt(p / (vocab * embed))
        step_size = LEARN_RATE * jnp.maximum(SCALE_FLOOR, param_rms) / jnp.maximum(1.0, update_rms / CLIP_LIMIT)
        line = lax.rsqrt(t.col_new[...]) * (jnp.sqrt(row_mean) * step_size)
        if t.is_emb:
            t.scale[...] = jnp.broadcast_to(line, t.scale.shape)
        else:
            t.scale[...] = jnp.transpose(jnp.broadcast_to(line, (LANES, LANES)))

    for k in range(AHEAD):
        load(k, emb)
    for t in (emb, head):
        for i, (src, dst) in enumerate(((t.param, t.pcopy), (t.row_old, t.row), (t.col_old, t.col))):
            pltpu.make_async_copy(src, dst, t.one.at[4 + i]).start()
        for acc in (t.col_acc, t.w_acc, t.r_acc, t.p_acc):
            acc[...] = jnp.zeros_like(acc)

    barrier = pltpu.get_barrier_semaphore()

    def greet(o, carry):
        to = lax.rem(me + o, others + 1)
        pl.semaphore_signal(barrier, inc=1, device_id=(to // nd, lax.rem(to, nd)), device_id_type=MESH)
        return carry

    lax.fori_loop(1, others + 1, greet, 0)
    pl.semaphore_wait(barrier, others)

    for k in range(AHEAD):
        exchange(k, emb)
    total = 2 * steps

    def both(k, act):
        @pl.when((k >= 0) & (k < steps))
        def _():
            act(k, emb)

        @pl.when((k >= steps) & (k < total))
        def _():
            act(k - steps, head)

    def fetch(k, t):
        load(k, t)
        exchange(k, t)

    def step(i, carry):
        both(i + AHEAD, fetch)
        both(i, first_hop)
        both(i - 1, second_hop)

        @pl.when(i == 2)
        def _():
            for t in (emb, head):
                arrived(t.pcopy, t.one.at[4])
                arrived(t.row, t.one.at[5])
                arrived(t.col, t.one.at[6])

        both(i - 3, finish)

        @pl.when(i == steps + 2)
        def _():
            send_cols(emb)

        @pl.when(i == total + 2)
        def _():
            send_cols(head)

        both(i - 4, functools.partial(row_hop, 1))
        both(i - 6, functools.partial(row_hop, 2))
        both(i - 8, complete)

        @pl.when(i == steps + 8)
        def _():
            send_scalars(emb)

        @pl.when(i == steps + 11)
        def _():
            finish_scalars(emb)

        return carry

    lax.fori_loop(0, total + 8, step, 0)
    send_scalars(head)
    finish_scalars(head)

    for t in (emb, head):
        arrived(t.half, t.snd.at[0])
        arrived(t.first_x, t.snd.at[1])
        arrived(t.first_y, t.snd.at[2])
        arrived(t.second_x, t.snd.at[3])
        arrived(t.second_y, t.snd.at[4])
        for s in range(3):
            arrived(t.rpart.at[s], t.snd.at[5 + s])
        arrived(t.colx.at[pl.ds(0, nz - 1)], t.one.at[0])
        arrived(t.scalx.at[pl.ds(0, others)], t.one.at[2])


def statistics(mesh, emb_grad, head_grad, emb_param, head_param, emb_row, emb_col, head_row, head_col):
    rows = emb_grad.shape[0]
    steps = rows // CHUNK
    nz, nd = mesh.shape["model"], mesh.shape["data"]
    f32 = jnp.float32

    def buffers(a, b):
        return [pltpu.VMEM((steps, 2, 2, a, b), f32), pltpu.VMEM((steps, 2, 2, a, b), f32),
                pltpu.VMEM((steps, 2, a // 2, b), f32), pltpu.VMEM((steps, 2, a // 2, b), f32),
                pltpu.VMEM((steps, a // 2, b), f32), pltpu.VMEM((steps, a // 2, b), f32)]

    def small(acc_rows):
        per = CHUNK // LANES
        return [pltpu.VMEM((3, steps, per, LANES), f32), pltpu.VMEM((3, steps, per, LANES), f32),
                pltpu.VMEM((acc_rows, LANES), f32), pltpu.VMEM((acc_rows, LANES), f32),
                pltpu.VMEM((per, LANES), f32), pltpu.VMEM((8, LANES), f32),
                pltpu.VMEM((nz, 1, LANES), f32), pltpu.VMEM((nz * nd, 1, LANES), f32), pltpu.VMEM((2, 1, LANES), f32),
                pltpu.VMEM((rows // LANES, LANES), f32), pltpu.VMEM((1, LANES), f32)]

    sems = [pltpu.SemaphoreType.DMA((steps,)) for _ in range(9)]
    sems += [pltpu.SemaphoreType.DMA((8,)), pltpu.SemaphoreType.DMA((7,))]

    def outs(shape, scale_rows):
        return [jax.ShapeDtypeStruct(shape, f32), jax.ShapeDtypeStruct(shape, f32),
                jax.ShapeDtypeStruct((rows // LANES, LANES), f32), jax.ShapeDtypeStruct((1, LANES), f32),
                jax.ShapeDtypeStruct((scale_rows, LANES), f32)]

    hbm = pl.BlockSpec(memory_space=pltpu.HBM)
    vmem = pl.BlockSpec(memory_space=pltpu.VMEM)
    results = pl.pallas_call(
        functools.partial(adafactor_kernel, steps, nz, nd),
        out_shape=outs((rows, LANES), 8) + outs((LANES, rows), LANES),
        in_specs=[hbm] * 8,
        out_specs=[vmem] * 10,
        scratch_shapes=(buffers(CHUNK, LANES) + buffers(LANES, CHUNK) + small(8) + small(LANES) + sems + sems),
        compiler_params=pltpu.CompilerParams(collective_id=0, has_side_effects=True, vmem_limit_bytes=VMEM_MIB * 2 ** 20),
    )(emb_grad, emb_param, emb_row.reshape(rows // LANES, LANES), emb_col.reshape(1, LANES),
      head_grad.reshape(2, 2, 2, LANES, rows), head_param, head_row.reshape(rows // LANES, LANES),
      head_col.reshape(1, LANES))
    return results[:5], results[5:]


PIECES = 8


def apply_kernel(rows, *refs):
    (emb_dir, emb_p, emb_r, emb_c, emb_s, head_dir, head_p, head_r, head_c, head_s,
     emb_new, emb_b16, head_new, head_b16, emb_ro, emb_co, head_ro, head_co,
     emb_tmp, emb_tmp16, head_tmp, head_tmp16, sem) = refs
    size = rows // PIECES

    def piece(j, carry):
        span = pl.ds(pl.multiple_of(j * size, size), size)
        new = emb_p[span, :] - emb_dir[span, :] * emb_s[0:1, :]
        emb_tmp[span, :] = new
        emb_tmp16[span, :] = new.astype(jnp.bfloat16)
        pltpu.make_async_copy(emb_tmp.at[span], emb_new.at[span], sem.at[0]).start()
        pltpu.make_async_copy(emb_tmp16.at[span], emb_b16.at[span], sem.at[1]).start()
        for i in range(size // LANES):
            cols = pl.ds(pl.multiple_of(j * size + i * LANES, LANES), LANES)
            new = head_p[:, cols] - head_dir[:, cols] * head_s[...]
            head_tmp[:, cols] = new
            head_tmp16[:, cols] = new.astype(jnp.bfloat16)
        pltpu.make_async_copy(head_tmp.at[:, span], head_new.at[:, span], sem.at[2]).start()
        pltpu.make_async_copy(head_tmp16.at[:, span], head_b16.at[:, span], sem.at[3]).start()
        return carry

    emb_ro[...] = emb_r[...]
    emb_co[...] = emb_c[...]
    head_ro[...] = head_r[...]
    head_co[...] = head_c[...]
    lax.fori_loop(0, PIECES, piece, 0)
    arrived(emb_new, sem.at[0])
    arrived(emb_b16, sem.at[1])
    arrived(head_new, sem.at[2])
    arrived(head_b16, sem.at[3])


def apply_update(emb, head):
    rows = emb[0].shape[0]
    f32, b16 = jnp.float32, jnp.bfloat16
    hbm = pl.BlockSpec(memory_space=pltpu.HBM)
    vmem = pl.BlockSpec(memory_space=pltpu.VMEM)
    shapes = ((rows, LANES), f32), ((rows, LANES), b16), ((LANES, rows), f32), ((LANES, rows), b16)
    small = ((rows // LANES, LANES), f32), ((1, LANES), f32)
    emb_new, emb_b16, head_new, head_b16, emb_r, emb_c, head_r, head_c = pl.pallas_call(
        functools.partial(apply_kernel, rows),
        out_shape=[jax.ShapeDtypeStruct(s, t) for s, t in shapes + small + small],
        in_specs=[vmem] * 10,
        out_specs=[hbm] * 4 + [vmem] * 4,
        scratch_shapes=[pltpu.VMEM(s, t) for s, t in shapes] + [pltpu.SemaphoreType.DMA((4,))],
        compiler_params=pltpu.CompilerParams(vmem_limit_bytes=24 * 2 ** 20),
    )(*emb, *head)
    return (emb_new, head_new, emb_r.reshape(rows), emb_c.reshape(LANES), head_r.reshape(rows), head_c.reshape(LANES),
            emb_b16, head_b16)


def solution(mesh):
    arg_specs = (P("model", "data"), P("data", "model"), P("data", "model", None), P("data", None, "model"),
                 P("model"), P("data"), P("model"), P("data"))
    result_specs = (P("model", "data"), P("data", "model"), P("model"), P("data"), P("model"), P("data"),
                    P("model", "data"), P("data", "model"))

    def local_step(emb_block, head_block, emb_contrib, head_contrib, emb_rows, emb_cols, head_rows, head_cols):
        emb, head = statistics(mesh, emb_contrib[0], head_contrib[0], emb_block, head_block,
                               emb_rows, emb_cols, head_rows, head_cols)
        return apply_update(emb, head)

    return jax.shard_map(local_step, mesh=mesh, in_specs=arg_specs, out_specs=result_specs, check_vma=False)
```

```python
import functools

import jax
import jax.numpy as jnp
from jax import lax
from jax.experimental import pallas as pl
from jax.experimental.pallas import tpu as pltpu
from jax.sharding import PartitionSpec as P

TRAIN_STEP = 10
DECAY_EXP = 0.8
EPS_ONE = 1e-30
CLIP_LIMIT = 1.0
SCALE_FLOOR = 1e-3
LEARN_RATE = float(TRAIN_STEP) ** -0.5
BETA_TWO = 1.0 - float(TRAIN_STEP) ** -DECAY_EXP

MESH = pl.DeviceIdType.MESH
UNIT = 128
BIG = 2
EMB_SMALLS = 2
HEAD_SMALLS = 2
AHEAD = 4
LAGS = (2, 4, 5, 7, 9)
LANES = 128
VMEM_MIB = 45
PSTART = 4
RELAYED = LAGS[4] + 4


class Table:
    def __init__(self, is_emb, units, grad, param, outs, bufs, small, sems):
        self.is_emb, self.grad, self.param = is_emb, grad, param
        self.smalls = EMB_SMALLS if is_emb else HEAD_SMALLS
        self.bigs = (units - self.smalls) // BIG
        self.chunks = self.smalls + self.bigs
        self.dirn, self.pcopy, self.row_new, self.col_new, self.scale = outs
        self.own, self.half, self.first_x, self.first_y, self.second_x, self.second_y = bufs
        (self.rpart, self.rrecv, self.rsum, self.rall, self.col_acc, self.w_acc, self.r_acc, self.p_acc, self.colx, self.scalx,
         self.vec) = small
        (self.ld, self.ra, self.rfx, self.rfy, self.rgx, self.rgy, self.rr0, self.rr1, self.rr2, self.snd, self.one) = sems
        self.rr = (self.rr0, self.rr1, self.rr2)

    def span(self, k):
        if self.is_emb:
            small = k < self.smalls
            return jnp.where(small, k, self.smalls + (k - self.smalls) * BIG), small
        small = k >= self.bigs
        return jnp.where(small, self.bigs * BIG + k - self.bigs, k * BIG), small

    def sized(self, k, act):
        first, small = self.span(k)

        @pl.when(small)
        def _():
            act(first, 1)

        @pl.when(jnp.logical_not(small))
        def _():
            act(first, BIG)

    def units(self, k, act):
        first, small = self.span(k)

        def one(j, carry):
            act(first + j)
            return carry

        lax.fori_loop(0, jnp.where(small, 1, BIG), one, 0)


N_OUT, N_BUF, N_SMALL, N_SEM = 5, 6, 11, 11
HALF = UNIT // 2


def arrived(ref, sem):
    pltpu.make_async_copy(ref, ref, sem).wait()


def lane_sum(a):
    return jnp.sum(a, axis=1, keepdims=True)


def fold8(a):
    return jnp.sum(a.reshape(a.shape[0] // 8, 8, a.shape[1]), axis=0)


def adafactor_kernel(units, nz, nd, *refs):
    emb_in, head_in, old = refs[0:2], refs[2:4], refs[4]
    pos = 5
    emb_out, head_out = refs[pos:pos + N_OUT], refs[pos + N_OUT:pos + 2 * N_OUT]
    pos += 2 * N_OUT
    emb_buf, head_buf = refs[pos:pos + N_BUF], refs[pos + N_BUF:pos + 2 * N_BUF]
    pos += 2 * N_BUF
    emb_small, head_small = refs[pos:pos + N_SMALL], refs[pos + N_SMALL:pos + 2 * N_SMALL]
    pos += 2 * N_SMALL
    emb_sem, head_sem = refs[pos:pos + N_SEM], refs[pos + N_SEM:pos + 2 * N_SEM]
    token, rall_sem, rall_snd = refs[pos + 2 * N_SEM:]
    emb = Table(True, units, *emb_in, emb_out, emb_buf, emb_small, emb_sem)
    head = Table(False, units, *head_in, head_out, head_buf, head_small, head_sem)
    vocab, embed = float(nz * units * UNIT), float(nd * LANES)
    others = nz * nd - 1
    bigs = head.bigs
    chunks = emb.chunks
    total = emb.chunks + head.chunks

    z = lax.axis_index("model")
    d = lax.axis_index("data")
    me = z * nd + d
    c = lax.rem(d, 2)
    x = lax.rem(d // 2, 2)
    y = d // 4
    partner = (z, d + 1 - 2 * c)
    xnbr = (z, d + 2 - 4 * x)
    ynbr = (z, d + 4 - 8 * y)
    ring = (partner, xnbr, ynbr)

    def send(src, dst, ssem, rsem, to):
        pltpu.make_async_remote_copy(src_ref=src, dst_ref=dst, send_sem=ssem, recv_sem=rsem,
                                     device_id=to, device_id_type=MESH).start()

    def blocks(t, u, n, core, buf):
        if t.is_emb:
            for yy in range(2):
                for xx in range(2):
                    col = pl.multiple_of(((yy * 2 + xx) * 2 + core) * LANES, LANES)
                    yield t.grad.at[pl.ds(u, n), :, pl.ds(col, LANES)], buf.at[pl.ds(u, n), yy, xx]
        else:
            for j in range(n):
                lanes = pl.ds(pl.multiple_of((u + j) * UNIT, UNIT), UNIT)
                yield t.grad.at[:, :, core, :, lanes], buf.at[u + j]

    def load(k, t):
        def act(u, n):
            for src, dst in blocks(t, u, n, c, t.own):
                pltpu.make_async_copy(src, dst, t.ld.at[k]).start()
        t.sized(k, act)

    def exchange(k, t):
        def act(u, n):
            for src, dst in blocks(t, u, n, 1 - c, t.half):
                send(src, dst, t.snd.at[0], t.ra.at[k], partner)
        t.sized(k, act)

    def first_hop(k, t):
        def act(u, n):
            part = pl.ds(u, n)
            arrived(t.own.at[part], t.ld.at[k])
            arrived(t.half.at[part], t.ra.at[k])
            for j in range(n):
                for yy in range(2):
                    t.own[u + j, yy, 1 - x, :HALF] += t.half[u + j, yy, 1 - x, :HALF]
            send(t.own.at[part, :, 1 - x, pl.ds(0, HALF)], t.first_x.at[part], t.snd.at[1], t.rfx.at[k], xnbr)
            for j in range(n):
                for xx in range(2):
                    t.own[u + j, 1 - y, xx, HALF:] += t.half[u + j, 1 - y, xx, HALF:]
            send(t.own.at[part, 1 - y, :, pl.ds(HALF, HALF)], t.first_y.at[part], t.snd.at[2], t.rfy.at[k], ynbr)
        t.sized(k, act)

    def second_hop(k, t):
        def act(u, n):
            part = pl.ds(u, n)
            arrived(t.first_x.at[part], t.rfx.at[k])
            for j in range(n):
                t.own[u + j, 1 - y, x, :HALF] += t.half[u + j, 1 - y, x, :HALF] + t.first_x[u + j, 1 - y]
            send(t.own.at[part, 1 - y, x, pl.ds(0, HALF)], t.second_x.at[part], t.snd.at[3], t.rgx.at[k], ynbr)
            arrived(t.first_y.at[part], t.rfy.at[k])
            for j in range(n):
                t.own[u + j, y, 1 - x, HALF:] += t.half[u + j, y, 1 - x, HALF:] + t.first_y[u + j, 1 - x]
            send(t.own.at[part, y, 1 - x, pl.ds(HALF, HALF)], t.second_y.at[part], t.snd.at[4], t.rgy.at[k], xnbr)
        t.sized(k, act)

    def tile(u):
        return pl.ds(pl.multiple_of(u * UNIT, UNIT), UNIT)

    def finish(k, t):
        def landed(u, n):
            arrived(t.second_x.at[pl.ds(u, n)], t.rgx.at[k])
            arrived(t.second_y.at[pl.ds(u, n)], t.rgy.at[k])

        def one(u):
            first = t.own[u, y, x, :HALF] + t.half[u, y, x, :HALF] + t.first_x[u, y] + t.second_x[u]
            last = t.own[u, y, x, HALF:] + t.half[u, y, x, HALF:] + t.first_y[u, x] + t.second_y[u]
            sq_first = first * first + EPS_ONE
            sq_last = last * last + EPS_ONE
            if t.is_emb:
                t.dirn[pl.ds(pl.multiple_of(u * UNIT, HALF), HALF), :] = first
                t.dirn[pl.ds(pl.multiple_of(u * UNIT + HALF, HALF), HALF), :] = last
                t.col_acc[...] += fold8(sq_first) + fold8(sq_last)
                sq = jnp.transpose(jnp.concatenate([sq_first, sq_last], axis=0))
                t.rpart[0, u] = jnp.sum(fold8(sq), axis=0, keepdims=True)
            else:
                t.dirn[:HALF, tile(u)] = first
                t.dirn[HALF:, tile(u)] = last
                t.col_acc[:HALF] += sq_first
                t.col_acc[HALF:] += sq_last
                t.rpart[0, u] = jnp.sum(fold8(sq_first) + fold8(sq_last), axis=0, keepdims=True)

        def pass_on(u, n):
            if not t.is_emb and n == 1:
                def to_peer(o, carry):
                    send(t.rpart.at[0, u], t.rall.at[k - bigs, d], rall_snd.at[0], rall_sem.at[k - bigs],
                         (z, lax.rem(d + o, nd)))
                    return carry
                lax.fori_loop(1, nd, to_peer, 0)
            else:
                send(t.rpart.at[0, pl.ds(u, n)], t.rrecv.at[0, pl.ds(u, n)], t.snd.at[5], t.rr[0].at[k], ring[0])

        t.sized(k, landed)
        t.units(k, one)
        t.sized(k, pass_on)

    def row_hop(s, k, t):
        def act(u, n):
            if t.is_emb or n > 1:
                part = pl.ds(u, n)
                arrived(t.rrecv.at[s - 1, part], t.rr[s - 1].at[k])
                t.rpart[s, part] = t.rpart[s - 1, part] + t.rrecv[s - 1, part]
                send(t.rpart.at[s, part], t.rrecv.at[s, part], t.snd.at[5 + s], t.rr[s].at[k], ring[s])
        t.sized(k, act)

    def complete(k, t):
        def landed(u, n):
            if not t.is_emb and n == 1:
                arrived(t.rall.at[k - bigs, pl.ds(0, nd - 1)], rall_sem.at[k - bigs])
                t.rall[k - bigs, d] = t.rpart[0, u]
                total = t.rall[k - bigs, 0]
                for i in range(1, nd):
                    total = total + t.rall[k - bigs, i]
                t.rsum[u] = total
            else:
                part = pl.ds(u, n)
                arrived(t.rrecv.at[2, part], t.rr[2].at[k])
                t.rsum[part] = t.rpart[2, part] + t.rrecv[2, part]

        def one(u):
            row = u if t.is_emb else units + u
            new = BETA_TWO * old[pl.ds(row, 1), :] + (1.0 - BETA_TWO) * (t.rsum[u] / embed)
            t.row_new[pl.ds(u, 1), :] = new
            t.r_acc[...] += new
            line = jnp.broadcast_to(lax.rsqrt(new), (LANES, LANES))
            if t.is_emb:
                n = t.dirn[tile(u), :] * jnp.transpose(line)
                t.dirn[tile(u), :] = n
                t.w_acc[...] += fold8(n * n)
                p = t.pcopy[tile(u), :]
            else:
                n = t.dirn[:, tile(u)] * line
                t.dirn[:, tile(u)] = n
                t.w_acc[...] += n * n
                p = t.pcopy[:, tile(u)]
            t.p_acc[...] += fold8(p * p)

        t.sized(k, landed)
        t.units(k, one)

    def per_col(t, acc):
        a = acc[...]
        return jnp.sum(a if t.is_emb else jnp.transpose(a), axis=0, keepdims=True)

    def send_cols(t):
        t.vec[0] = per_col(t, t.col_acc)
        for o in range(1, nz):
            send(t.vec.at[0], t.colx.at[z], t.one.at[0], t.one.at[1], (lax.rem(z + o, nz), d))

    def send_scalars(t):
        arrived(t.colx.at[pl.ds(0, nz - 1)], t.one.at[1])
        t.colx[z] = t.vec[0]
        col_sq = t.colx[0]
        for i in range(1, nz):
            col_sq = col_sq + t.colx[i]
        at = 2 * units + (0 if t.is_emb else 1)
        new = BETA_TWO * old[at:at + 1, :] + (1.0 - BETA_TWO) * (col_sq / vocab)
        t.col_new[...] = new
        w = lane_sum(per_col(t, t.w_acc) / new)
        r = lane_sum(t.r_acc[...]) / nd
        p = lane_sum(jnp.sum(t.p_acc[...], axis=0, keepdims=True))
        lane = lax.broadcasted_iota(jnp.int32, (1, LANES), 1)
        t.vec[1] = jnp.where(lane == 0, w, jnp.where(lane == 1, r, jnp.where(lane == 2, p, 0.0)))

        def one(o, carry):
            to = lax.rem(me + o, others + 1)
            send(t.vec.at[1], t.scalx.at[me], t.one.at[2], t.one.at[3], (to // nd, lax.rem(to, nd)))
            return carry

        lax.fori_loop(1, others + 1, one, 0)

    def finish_scalars(t):
        arrived(t.scalx.at[pl.ds(0, others)], t.one.at[3])
        t.scalx[me] = t.vec[1]
        total = jnp.sum(t.scalx[...], axis=0)
        lane = lax.broadcasted_iota(jnp.int32, (1, LANES), 1)
        w, r, p = (lane_sum(jnp.where(lane == i, total, 0.0)) for i in range(3))
        row_mean = r / vocab
        update_rms = jnp.sqrt(w * row_mean / (vocab * embed))
        param_rms = jnp.sqrt(p / (vocab * embed))
        step_size = LEARN_RATE * jnp.maximum(SCALE_FLOOR, param_rms) / jnp.maximum(1.0, update_rms / CLIP_LIMIT)
        line = lax.rsqrt(t.col_new[...]) * (jnp.sqrt(row_mean) * step_size)
        if t.is_emb:
            t.scale[...] = jnp.broadcast_to(line, t.scale.shape)
        else:
            t.scale[...] = jnp.transpose(jnp.broadcast_to(line, (LANES, LANES)))

    barrier = pltpu.get_barrier_semaphore()
    above, below = (lax.rem(z + 1, nz), d), (lax.rem(z + nz - 1, nz), d)

    def greet(to):
        pl.semaphore_signal(barrier, inc=1, device_id=to, device_id_type=MESH)

    for peer in ring:
        greet(peer)

    @pl.when(z < nz - 1)
    def _():
        greet(above)

    @pl.when(z > 0)
    def _():
        greet(below)

    for k in range(AHEAD):
        load(k, emb)
    for t in (emb, head):
        for acc in (t.col_acc, t.w_acc, t.r_acc, t.p_acc):
            acc[...] = jnp.zeros_like(acc)
    pl.semaphore_wait(barrier, 3 + jnp.where(z < nz - 1, 1, 0) + jnp.where(z > 0, 1, 0))

    for k in range(AHEAD):
        exchange(k, emb)

    def both(k, act):
        @pl.when((k >= 0) & (k < chunks))
        def _():
            act(k, emb)

        @pl.when((k >= chunks) & (k < total))
        def _():
            act(k - chunks, head)

    def fetch(k, t):
        load(k, t)
        exchange(k, t)

    def relay(r):
        for turn, source, last, to, sem in ((z, 0, nz - 1, above, token.at[0]), (nz - 1 - z, nz - 1, 0, below, token.at[1])):
            @pl.when(r == turn)
            def _():
                @pl.when(z != source)
                def _():
                    pl.semaphore_wait(sem, 1)

                @pl.when(z != last)
                def _():
                    pl.semaphore_signal(sem, inc=1, device_id=to, device_id_type=MESH)

    def step(i, carry):
        both(i + AHEAD, fetch)
        both(i, first_hop)

        @pl.when(i == PSTART)
        def _():
            for t in (emb, head):
                pltpu.make_async_copy(t.param, t.pcopy, t.one.at[4]).start()

        both(i - LAGS[0], second_hop)

        @pl.when(i == LAGS[4] - 1)
        def _():
            for t in (emb, head):
                arrived(t.pcopy, t.one.at[4])

        both(i - LAGS[1], finish)
        relay(i - LAGS[4] - 1)

        @pl.when(i == chunks - 1 + RELAYED)
        def _():
            send_cols(emb)

        @pl.when(i == total - 1 + LAGS[1])
        def _():
            send_cols(head)

        both(i - LAGS[2], functools.partial(row_hop, 1))
        both(i - LAGS[3], functools.partial(row_hop, 2))
        both(i - LAGS[4], complete)

        @pl.when(i == chunks + RELAYED)
        def _():
            send_scalars(emb)

        @pl.when(i == chunks + RELAYED + 2)
        def _():
            finish_scalars(emb)

        return carry

    lax.fori_loop(0, total + LAGS[4], step, 0)
    send_scalars(head)
    finish_scalars(head)

    for t in (emb, head):
        arrived(t.half, t.snd.at[0])
        arrived(t.first_x, t.snd.at[1])
        arrived(t.first_y, t.snd.at[2])
        arrived(t.second_x, t.snd.at[3])
        arrived(t.second_y, t.snd.at[4])
        hopped = t.rpart if t.is_emb else t.rpart.at[:, pl.ds(0, bigs * BIG)]
        for s in range(3):
            arrived(hopped.at[s], t.snd.at[5 + s])
        arrived(t.colx.at[pl.ds(0, nz - 1)], t.one.at[0])
        arrived(t.scalx.at[pl.ds(0, others)], t.one.at[2])
    arrived(head.rall.at[:, pl.ds(0, nd - 1)], rall_snd.at[0])


def statistics(mesh, emb_grad, head_grad, emb_param, head_param, emb_row, emb_col, head_row, head_col):
    rows, embed = emb_grad.shape
    units = rows // UNIT
    nz, nd = mesh.shape["model"], mesh.shape["data"]
    f32 = jnp.float32
    old = jnp.concatenate([a.reshape(a.shape[0] // LANES, LANES) for a in (emb_row, head_row, emb_col, head_col)])

    buffers = [pltpu.VMEM((units, 2, 2, UNIT, LANES), f32), pltpu.VMEM((units, 2, 2, UNIT, LANES), f32),
               pltpu.VMEM((units, 2, HALF, LANES), f32), pltpu.VMEM((units, 2, HALF, LANES), f32),
               pltpu.VMEM((units, HALF, LANES), f32), pltpu.VMEM((units, HALF, LANES), f32)]

    def small(acc_rows):
        return [pltpu.VMEM((3, units, 1, LANES), f32), pltpu.VMEM((3, units, 1, LANES), f32),
                pltpu.VMEM((units, 1, LANES), f32), pltpu.VMEM((HEAD_SMALLS, nd, 1, LANES), f32),
                pltpu.VMEM((acc_rows, LANES), f32), pltpu.VMEM((acc_rows, LANES), f32),
                pltpu.VMEM((1, LANES), f32), pltpu.VMEM((8, LANES), f32),
                pltpu.VMEM((nz, 1, LANES), f32), pltpu.VMEM((nz * nd, 1, LANES), f32), pltpu.VMEM((2, 1, LANES), f32)]

    sems = [pltpu.SemaphoreType.DMA((units // BIG + 2,)) for _ in range(9)]
    sems += [pltpu.SemaphoreType.DMA((8,)), pltpu.SemaphoreType.DMA((5,))]

    def outs(shape, scale_rows):
        return [jax.ShapeDtypeStruct(shape, f32), jax.ShapeDtypeStruct(shape, f32),
                jax.ShapeDtypeStruct((units, LANES), f32), jax.ShapeDtypeStruct((1, LANES), f32),
                jax.ShapeDtypeStruct((scale_rows, LANES), f32)]

    hbm = pl.BlockSpec(memory_space=pltpu.HBM)
    vmem = pl.BlockSpec(memory_space=pltpu.VMEM)
    results = pl.pallas_call(
        functools.partial(adafactor_kernel, units, nz, nd),
        out_shape=outs((rows, LANES), 8) + outs((LANES, rows), LANES),
        in_specs=[hbm] * 4 + [vmem],
        out_specs=[vmem] * 10,
        scratch_shapes=(buffers + buffers + small(8) + small(LANES) + sems + sems
                        + [pltpu.SemaphoreType.REGULAR((2,)), pltpu.SemaphoreType.DMA((HEAD_SMALLS,)),
                           pltpu.SemaphoreType.DMA((1,))]),
        compiler_params=pltpu.CompilerParams(collective_id=0, has_side_effects=True, vmem_limit_bytes=VMEM_MIB * 2 ** 20),
    )(emb_grad.reshape(units, UNIT, embed), emb_param, head_grad.reshape(2, 2, 2, LANES, rows), head_param, old)
    return results[:5], results[5:]


PIECES = 8


def apply_kernel(rows, *refs):
    (emb_dir, emb_p, emb_r, emb_c, emb_s, head_dir, head_p, head_r, head_c, head_s,
     emb_new, emb_b16, head_new, head_b16, emb_ro, emb_co, head_ro, head_co,
     emb_tmp, emb_tmp16, head_tmp, head_tmp16, sem) = refs
    size = rows // PIECES

    def piece(j, carry):
        span = pl.ds(pl.multiple_of(j * size, size), size)
        new = emb_p[span, :] - emb_dir[span, :] * emb_s[0:1, :]
        emb_tmp[span, :] = new
        emb_tmp16[span, :] = new.astype(jnp.bfloat16)
        pltpu.make_async_copy(emb_tmp.at[span], emb_new.at[span], sem.at[0]).start()
        pltpu.make_async_copy(emb_tmp16.at[span], emb_b16.at[span], sem.at[1]).start()
        for i in range(size // LANES):
            cols = pl.ds(pl.multiple_of(j * size + i * LANES, LANES), LANES)
            new = head_p[:, cols] - head_dir[:, cols] * head_s[...]
            head_tmp[:, cols] = new
            head_tmp16[:, cols] = new.astype(jnp.bfloat16)
        pltpu.make_async_copy(head_tmp.at[:, span], head_new.at[:, span], sem.at[2]).start()
        pltpu.make_async_copy(head_tmp16.at[:, span], head_b16.at[:, span], sem.at[3]).start()
        return carry

    emb_ro[...] = emb_r[...]
    emb_co[...] = emb_c[...]
    head_ro[...] = head_r[...]
    head_co[...] = head_c[...]
    lax.fori_loop(0, PIECES, piece, 0)
    arrived(emb_new, sem.at[0])
    arrived(emb_b16, sem.at[1])
    arrived(head_new, sem.at[2])
    arrived(head_b16, sem.at[3])


def apply_update(emb, head):
    rows = emb[0].shape[0]
    f32, b16 = jnp.float32, jnp.bfloat16
    hbm = pl.BlockSpec(memory_space=pltpu.HBM)
    vmem = pl.BlockSpec(memory_space=pltpu.VMEM)
    shapes = ((rows, LANES), f32), ((rows, LANES), b16), ((LANES, rows), f32), ((LANES, rows), b16)
    small = ((rows // LANES, LANES), f32), ((1, LANES), f32)
    emb_new, emb_b16, head_new, head_b16, emb_r, emb_c, head_r, head_c = pl.pallas_call(
        functools.partial(apply_kernel, rows),
        out_shape=[jax.ShapeDtypeStruct(s, t) for s, t in shapes + small + small],
        in_specs=[vmem] * 10,
        out_specs=[hbm] * 4 + [vmem] * 4,
        scratch_shapes=[pltpu.VMEM(s, t) for s, t in shapes] + [pltpu.SemaphoreType.DMA((4,))],
        compiler_params=pltpu.CompilerParams(vmem_limit_bytes=24 * 2 ** 20),
    )(*emb, *head)
    return (emb_new, head_new, emb_r.reshape(rows), emb_c.reshape(LANES), head_r.reshape(rows), head_c.reshape(LANES),
            emb_b16, head_b16)


def solution(mesh):
    arg_specs = (P("model", "data"), P("data", "model"), P("data", "model", None), P("data", None, "model"),
                 P("model"), P("data"), P("model"), P("data"))
    result_specs = (P("model", "data"), P("data", "model"), P("model"), P("data"), P("model"), P("data"),
                    P("model", "data"), P("data", "model"))

    def local_step(emb_block, head_block, emb_contrib, head_contrib, emb_rows, emb_cols, head_rows, head_cols):
        emb, head = statistics(mesh, emb_contrib[0], head_contrib[0], emb_block, head_block,
                               emb_rows, emb_cols, head_rows, head_cols)
        return apply_update(emb, head)

    return jax.shard_map(local_step, mesh=mesh, in_specs=arg_specs, out_specs=result_specs, check_vma=False)
```

```python
import functools

import jax
import jax.numpy as jnp
from jax import lax
from jax.experimental import pallas as pl
from jax.experimental.pallas import tpu as pltpu
from jax.sharding import PartitionSpec as P

TRAIN_STEP = 10
DECAY_EXP = 0.8
EPS_ONE = 1e-30
CLIP_LIMIT = 1.0
SCALE_FLOOR = 1e-3
LEARN_RATE = float(TRAIN_STEP) ** -0.5
BETA_TWO = 1.0 - float(TRAIN_STEP) ** -DECAY_EXP

MESH = pl.DeviceIdType.MESH
UNIT = 128
BIG = 4
EMB_SMALLS = 4
HEAD_SMALLS = 8
DIRECT = 8
AHEAD = 4
LAGS = (2, 4, 5, 7, 9)
LANES = 128
VMEM_MIB = 45
PSTART = 4
RELAYED = LAGS[4] + 4


class Table:
    def __init__(self, is_emb, units, grad, param, outs, bufs, small, sems):
        self.is_emb, self.grad, self.param = is_emb, grad, param
        self.smalls = EMB_SMALLS if is_emb else HEAD_SMALLS
        self.bigs = (units - self.smalls) // BIG
        self.chunks = self.smalls + self.bigs
        self.hops = self.chunks if is_emb else self.chunks - DIRECT
        self.dirn, self.pcopy, self.row_new, self.col_new, self.scale = outs
        self.own, self.half, self.first_x, self.first_y, self.second_x, self.second_y = bufs
        (self.rpart, self.rrecv, self.rsum, self.rall, self.col_acc, self.w_acc, self.r_acc, self.p_acc, self.colx, self.scalx,
         self.vec) = small
        (self.ld, self.ra, self.rfx, self.rfy, self.rgx, self.rgy, self.rr0, self.rr1, self.rr2, self.snd, self.one) = sems
        self.rr = (self.rr0, self.rr1, self.rr2)

    def span(self, k):
        if self.is_emb:
            small = k < self.smalls
            return jnp.where(small, k, self.smalls + (k - self.smalls) * BIG), small
        small = k >= self.bigs
        return jnp.where(small, self.bigs * BIG + k - self.bigs, k * BIG), small

    def sized(self, k, act, when=True):
        first, small = self.span(k)

        @pl.when(small & when)
        def _():
            act(first, 1)

        @pl.when(jnp.logical_not(small) & when)
        def _():
            act(first, BIG)

    def units(self, k, act):
        first, small = self.span(k)

        def one(j, carry):
            act(first + j)
            return carry

        lax.fori_loop(0, jnp.where(small, 1, BIG), one, 0)


N_OUT, N_BUF, N_SMALL, N_SEM = 5, 6, 11, 11
HALF = UNIT // 2


def arrived(ref, sem):
    pltpu.make_async_copy(ref, ref, sem).wait()


def lane_sum(a):
    return jnp.sum(a, axis=1, keepdims=True)


def fold8(a):
    return jnp.sum(a.reshape(a.shape[0] // 8, 8, a.shape[1]), axis=0)


def adafactor_kernel(units, nz, nd, *refs):
    emb_in, head_in, old_in = refs[0:2], refs[2:4], refs[4:8]
    pos = 8
    emb_out, head_out = refs[pos:pos + N_OUT], refs[pos + N_OUT:pos + 2 * N_OUT]
    pos += 2 * N_OUT
    emb_buf, head_buf = refs[pos:pos + N_BUF], refs[pos + N_BUF:pos + 2 * N_BUF]
    pos += 2 * N_BUF
    emb_small, head_small = refs[pos:pos + N_SMALL], refs[pos + N_SMALL:pos + 2 * N_SMALL]
    pos += 2 * N_SMALL
    emb_sem, head_sem = refs[pos:pos + N_SEM], refs[pos + N_SEM:pos + 2 * N_SEM]
    token, rall_sem, rall_snd, old, old_sem = refs[pos + 2 * N_SEM:]
    emb = Table(True, units, *emb_in, emb_out, emb_buf, emb_small, emb_sem)
    head = Table(False, units, *head_in, head_out, head_buf, head_small, head_sem)
    vocab, embed = float(nz * units * UNIT), float(nd * LANES)
    others = nz * nd - 1
    old_rows = (0, units), (units, units), (2 * units, 1), (2 * units + 1, 1)
    hop_units = head.hops * BIG
    chunks = emb.chunks
    total = emb.chunks + head.chunks

    z = lax.axis_index("model")
    d = lax.axis_index("data")
    me = z * nd + d
    c = lax.rem(d, 2)
    x = lax.rem(d // 2, 2)
    y = d // 4
    partner = (z, d + 1 - 2 * c)
    xnbr = (z, d + 2 - 4 * x)
    ynbr = (z, d + 4 - 8 * y)
    ring = (partner, xnbr, ynbr)

    def send(src, dst, ssem, rsem, to):
        pltpu.make_async_remote_copy(src_ref=src, dst_ref=dst, send_sem=ssem, recv_sem=rsem,
                                     device_id=to, device_id_type=MESH).start()

    def blocks(t, u, n, core, buf):
        if t.is_emb:
            for yy in range(2):
                for xx in range(2):
                    col = pl.multiple_of(((yy * 2 + xx) * 2 + core) * LANES, LANES)
                    yield t.grad.at[pl.ds(u, n), :, pl.ds(col, LANES)], buf.at[pl.ds(u, n), yy, xx]
        else:
            for j in range(n):
                lanes = pl.ds(pl.multiple_of((u + j) * UNIT, UNIT), UNIT)
                yield t.grad.at[:, :, core, :, lanes], buf.at[u + j]

    def load(k, t):
        def act(u, n):
            for src, dst in blocks(t, u, n, c, t.own):
                pltpu.make_async_copy(src, dst, t.ld.at[k]).start()
        t.sized(k, act)

    def exchange(k, t):
        def act(u, n):
            for src, dst in blocks(t, u, n, 1 - c, t.half):
                send(src, dst, t.snd.at[0], t.ra.at[k], partner)
        t.sized(k, act)

    def first_hop(k, t):
        def act(u, n):
            part = pl.ds(u, n)
            arrived(t.own.at[part], t.ld.at[k])
            arrived(t.half.at[part], t.ra.at[k])
            for j in range(n):
                for yy in range(2):
                    t.own[u + j, yy, 1 - x, :HALF] += t.half[u + j, yy, 1 - x, :HALF]
            send(t.own.at[part, :, 1 - x, pl.ds(0, HALF)], t.first_x.at[part], t.snd.at[1], t.rfx.at[k], xnbr)
            for j in range(n):
                for xx in range(2):
                    t.own[u + j, 1 - y, xx, HALF:] += t.half[u + j, 1 - y, xx, HALF:]
            send(t.own.at[part, 1 - y, :, pl.ds(HALF, HALF)], t.first_y.at[part], t.snd.at[2], t.rfy.at[k], ynbr)
        t.sized(k, act)

    def second_hop(k, t):
        def act(u, n):
            part = pl.ds(u, n)
            arrived(t.first_x.at[part], t.rfx.at[k])
            for j in range(n):
                t.own[u + j, 1 - y, x, :HALF] += t.half[u + j, 1 - y, x, :HALF] + t.first_x[u + j, 1 - y]
            send(t.own.at[part, 1 - y, x, pl.ds(0, HALF)], t.second_x.at[part], t.snd.at[3], t.rgx.at[k], ynbr)
            arrived(t.first_y.at[part], t.rfy.at[k])
            for j in range(n):
                t.own[u + j, y, 1 - x, HALF:] += t.half[u + j, y, 1 - x, HALF:] + t.first_y[u + j, 1 - x]
            send(t.own.at[part, y, 1 - x, pl.ds(HALF, HALF)], t.second_y.at[part], t.snd.at[4], t.rgy.at[k], xnbr)
        t.sized(k, act)

    def tile(u):
        return pl.ds(pl.multiple_of(u * UNIT, UNIT), UNIT)

    def finish(k, t):
        def landed(u, n):
            arrived(t.second_x.at[pl.ds(u, n)], t.rgx.at[k])
            arrived(t.second_y.at[pl.ds(u, n)], t.rgy.at[k])

        def one(u):
            first = t.own[u, y, x, :HALF] + t.half[u, y, x, :HALF] + t.first_x[u, y] + t.second_x[u]
            last = t.own[u, y, x, HALF:] + t.half[u, y, x, HALF:] + t.first_y[u, x] + t.second_y[u]
            sq_first = first * first + EPS_ONE
            sq_last = last * last + EPS_ONE
            if t.is_emb:
                t.dirn[pl.ds(pl.multiple_of(u * UNIT, HALF), HALF), :] = first
                t.dirn[pl.ds(pl.multiple_of(u * UNIT + HALF, HALF), HALF), :] = last
                t.col_acc[...] += fold8(sq_first) + fold8(sq_last)
                sq = jnp.transpose(jnp.concatenate([sq_first, sq_last], axis=0))
                t.rpart[0, u] = jnp.sum(fold8(sq), axis=0, keepdims=True)
            else:
                t.dirn[:HALF, tile(u)] = first
                t.dirn[HALF:, tile(u)] = last
                t.col_acc[:HALF] += sq_first
                t.col_acc[HALF:] += sq_last
                t.rpart[0, u] = jnp.sum(fold8(sq_first) + fold8(sq_last), axis=0, keepdims=True)

        def pass_on(u, n):
            send(t.rpart.at[0, pl.ds(u, n)], t.rrecv.at[0, pl.ds(u, n)], t.snd.at[5], t.rr[0].at[k], ring[0])

        def to_all(u, n):
            def to_peer(o, carry):
                send(t.rpart.at[0, pl.ds(u, n)], t.rall.at[d, pl.ds(u - hop_units, n)], rall_snd.at[0],
                     rall_sem.at[k - t.hops], (z, lax.rem(d + o, nd)))
                return carry
            lax.fori_loop(1, nd, to_peer, 0)

        t.sized(k, landed)
        t.units(k, one)
        t.sized(k, pass_on, k < t.hops)
        if not t.is_emb:
            t.sized(k, to_all, k >= t.hops)

    def row_hop(s, k, t):
        def act(u, n):
            part = pl.ds(u, n)
            arrived(t.rrecv.at[s - 1, part], t.rr[s - 1].at[k])
            t.rpart[s, part] = t.rpart[s - 1, part] + t.rrecv[s - 1, part]
            send(t.rpart.at[s, part], t.rrecv.at[s, part], t.snd.at[5 + s], t.rr[s].at[k], ring[s])
        t.sized(k, act, k < t.hops)

    def complete(k, t):
        def landed(u, n):
            part = pl.ds(u, n)
            arrived(t.rrecv.at[2, part], t.rr[2].at[k])
            t.rsum[part] = t.rpart[2, part] + t.rrecv[2, part]

        def landed_all(u, n):
            part = pl.ds(u - hop_units, n)
            arrived(t.rall.at[pl.ds(0, nd - 1), part], rall_sem.at[k - t.hops])
            t.rall[d, part] = t.rpart[0, pl.ds(u, n)]
            t.rsum[pl.ds(u, n)] = jnp.sum(t.rall[:, part], axis=0)

        def one(u):
            row = u if t.is_emb else units + u
            new = BETA_TWO * old[pl.ds(row, 1), :] + (1.0 - BETA_TWO) * (t.rsum[u] / embed)
            t.row_new[pl.ds(u, 1), :] = new
            t.r_acc[...] += new
            line = jnp.broadcast_to(lax.rsqrt(new), (LANES, LANES))
            if t.is_emb:
                n = t.dirn[tile(u), :] * jnp.transpose(line)
                t.dirn[tile(u), :] = n
                t.w_acc[...] += fold8(n * n)
                p = t.pcopy[tile(u), :]
            else:
                n = t.dirn[:, tile(u)] * line
                t.dirn[:, tile(u)] = n
                t.w_acc[...] += n * n
                p = t.pcopy[:, tile(u)]
            t.p_acc[...] += fold8(p * p)

        t.sized(k, landed, k < t.hops)
        if not t.is_emb:
            t.sized(k, landed_all, k >= t.hops)
        t.units(k, one)

    def per_col(t, acc):
        a = acc[...]
        return jnp.sum(a if t.is_emb else jnp.transpose(a), axis=0, keepdims=True)

    def send_cols(t):
        t.vec[0] = per_col(t, t.col_acc)
        for o in range(1, nz):
            send(t.vec.at[0], t.colx.at[z], t.one.at[0], t.one.at[1], (lax.rem(z + o, nz), d))

    def send_scalars(t):
        arrived(t.colx.at[pl.ds(0, nz - 1)], t.one.at[1])
        t.colx[z] = t.vec[0]
        col_sq = t.colx[0]
        for i in range(1, nz):
            col_sq = col_sq + t.colx[i]
        at = 2 * units + (0 if t.is_emb else 1)
        new = BETA_TWO * old[at:at + 1, :] + (1.0 - BETA_TWO) * (col_sq / vocab)
        t.col_new[...] = new
        w = lane_sum(per_col(t, t.w_acc) / new)
        r = lane_sum(t.r_acc[...]) / nd
        p = lane_sum(jnp.sum(t.p_acc[...], axis=0, keepdims=True))
        lane = lax.broadcasted_iota(jnp.int32, (1, LANES), 1)
        t.vec[1] = jnp.where(lane == 0, w, jnp.where(lane == 1, r, jnp.where(lane == 2, p, 0.0)))

        def one(o, carry):
            far = o // nd
            plane = jnp.where(z < nz // 2, nz - 1 - far, far)
            peer = lax.rem(d + o, nd)

            @pl.when(plane * nd + peer != me)
            def _():
                send(t.vec.at[1], t.scalx.at[me], t.one.at[2], t.one.at[3], (plane, peer))
            return carry

        lax.fori_loop(0, others + 1, one, 0)

    def finish_scalars(t):
        arrived(t.scalx.at[pl.ds(0, others)], t.one.at[3])
        t.scalx[me] = t.vec[1]
        total = jnp.sum(t.scalx[...], axis=0)
        lane = lax.broadcasted_iota(jnp.int32, (1, LANES), 1)
        w, r, p = (lane_sum(jnp.where(lane == i, total, 0.0)) for i in range(3))
        row_mean = r / vocab
        update_rms = jnp.sqrt(w * row_mean / (vocab * embed))
        param_rms = jnp.sqrt(p / (vocab * embed))
        step_size = LEARN_RATE * jnp.maximum(SCALE_FLOOR, param_rms) / jnp.maximum(1.0, update_rms / CLIP_LIMIT)
        line = lax.rsqrt(t.col_new[...]) * (jnp.sqrt(row_mean) * step_size)
        if t.is_emb:
            t.scale[...] = jnp.broadcast_to(line, t.scale.shape)
        else:
            t.scale[...] = jnp.transpose(jnp.broadcast_to(line, (LANES, LANES)))

    barrier = pltpu.get_barrier_semaphore()
    above, below = (lax.rem(z + 1, nz), d), (lax.rem(z + nz - 1, nz), d)

    def greet(to):
        pl.semaphore_signal(barrier, inc=1, device_id=to, device_id_type=MESH)

    for peer in ring:
        greet(peer)

    @pl.when(z < nz - 1)
    def _():
        greet(above)

    @pl.when(z > 0)
    def _():
        greet(below)

    for k in range(AHEAD):
        load(k, emb)
    for t in (emb, head):
        for acc in (t.col_acc, t.w_acc, t.r_acc, t.p_acc):
            acc[...] = jnp.zeros_like(acc)
    pl.semaphore_wait(barrier, 3 + jnp.where(z < nz - 1, 1, 0) + jnp.where(z > 0, 1, 0))

    for k in range(AHEAD):
        exchange(k, emb)

    def both(k, act):
        @pl.when((k >= 0) & (k < chunks))
        def _():
            act(k, emb)

        @pl.when((k >= chunks) & (k < total))
        def _():
            act(k - chunks, head)

    def fetch(k, t):
        load(k, t)
        exchange(k, t)

    def relay(r):
        for turn, source, last, to, sem in ((z, 0, nz - 1, above, token.at[0]), (nz - 1 - z, nz - 1, 0, below, token.at[1])):
            @pl.when(r == turn)
            def _():
                @pl.when(z != source)
                def _():
                    pl.semaphore_wait(sem, 1)

                @pl.when(z != last)
                def _():
                    pl.semaphore_signal(sem, inc=1, device_id=to, device_id_type=MESH)

    def step(i, carry):
        both(i + AHEAD, fetch)
        both(i, first_hop)

        @pl.when(i == PSTART)
        def _():
            for t in (emb, head):
                pltpu.make_async_copy(t.param, t.pcopy, t.one.at[4]).start()
            for i, (first, n) in enumerate(old_rows):
                pltpu.make_async_copy(old_in[i], old.at[pl.ds(first, n)], old_sem.at[i]).start()

        both(i - LAGS[0], second_hop)

        @pl.when(i == LAGS[4] - 1)
        def _():
            for t in (emb, head):
                arrived(t.pcopy, t.one.at[4])
            for i, (first, n) in enumerate(old_rows):
                arrived(old.at[pl.ds(first, n)], old_sem.at[i])

        both(i - LAGS[1], finish)
        relay(i - LAGS[4] - 1)

        @pl.when(i == chunks - 1 + RELAYED)
        def _():
            send_cols(emb)

        @pl.when(i == total - 1 + LAGS[1])
        def _():
            send_cols(head)

        both(i - LAGS[2], functools.partial(row_hop, 1))
        both(i - LAGS[3], functools.partial(row_hop, 2))
        both(i - LAGS[4], complete)

        @pl.when(i == chunks + RELAYED)
        def _():
            send_scalars(emb)

        @pl.when(i == chunks + RELAYED + 2)
        def _():
            finish_scalars(emb)

        return carry

    lax.fori_loop(0, total + LAGS[4], step, 0)
    send_scalars(head)
    finish_scalars(head)

    for t in (emb, head):
        arrived(t.half, t.snd.at[0])
        arrived(t.first_x, t.snd.at[1])
        arrived(t.first_y, t.snd.at[2])
        arrived(t.second_x, t.snd.at[3])
        arrived(t.second_y, t.snd.at[4])
        hopped = t.rpart if t.is_emb else t.rpart.at[:, pl.ds(0, hop_units)]
        for s in range(3):
            arrived(hopped.at[s], t.snd.at[5 + s])
        arrived(t.colx.at[pl.ds(0, nz - 1)], t.one.at[0])
        arrived(t.scalx.at[pl.ds(0, others)], t.one.at[2])
    arrived(head.rall.at[pl.ds(0, nd - 1)], rall_snd.at[0])


def statistics(mesh, emb_grad, head_grad, emb_param, head_param, emb_row, emb_col, head_row, head_col):
    rows, embed = emb_grad.shape
    units = rows // UNIT
    chunks = max(s + (units - s) // BIG for s in (EMB_SMALLS, HEAD_SMALLS))
    nz, nd = mesh.shape["model"], mesh.shape["data"]
    f32 = jnp.float32
    old = [pltpu.with_memory_space_constraint(a.reshape(a.shape[0] // LANES, LANES), pltpu.HBM)
           for a in (emb_row, head_row, emb_col, head_col)]

    buffers = [pltpu.VMEM((units, 2, 2, UNIT, LANES), f32), pltpu.VMEM((units, 2, 2, UNIT, LANES), f32),
               pltpu.VMEM((units, 2, HALF, LANES), f32), pltpu.VMEM((units, 2, HALF, LANES), f32),
               pltpu.VMEM((units, HALF, LANES), f32), pltpu.VMEM((units, HALF, LANES), f32)]

    def small(acc_rows):
        return [pltpu.VMEM((3, units, 1, LANES), f32), pltpu.VMEM((3, units, 1, LANES), f32),
                pltpu.VMEM((units, 1, LANES), f32), pltpu.VMEM((nd, HEAD_SMALLS + (DIRECT - HEAD_SMALLS) * BIG, 1, LANES), f32),
                pltpu.VMEM((acc_rows, LANES), f32), pltpu.VMEM((acc_rows, LANES), f32),
                pltpu.VMEM((1, LANES), f32), pltpu.VMEM((8, LANES), f32),
                pltpu.VMEM((nz, 1, LANES), f32), pltpu.VMEM((nz * nd, 1, LANES), f32), pltpu.VMEM((2, 1, LANES), f32)]

    sems = [pltpu.SemaphoreType.DMA((chunks,)) for _ in range(9)]
    sems += [pltpu.SemaphoreType.DMA((8,)), pltpu.SemaphoreType.DMA((5,))]

    def outs(shape, scale_rows):
        return [jax.ShapeDtypeStruct(shape, f32), jax.ShapeDtypeStruct(shape, f32),
                jax.ShapeDtypeStruct((units, LANES), f32), jax.ShapeDtypeStruct((1, LANES), f32),
                jax.ShapeDtypeStruct((scale_rows, LANES), f32)]

    hbm = pl.BlockSpec(memory_space=pltpu.HBM)
    vmem = pl.BlockSpec(memory_space=pltpu.VMEM)
    results = pl.pallas_call(
        functools.partial(adafactor_kernel, units, nz, nd),
        out_shape=outs((rows, LANES), 8) + outs((LANES, rows), LANES),
        in_specs=[hbm] * 8,
        out_specs=[vmem] * 10,
        scratch_shapes=(buffers + buffers + small(8) + small(LANES) + sems + sems
                        + [pltpu.SemaphoreType.REGULAR((2,)), pltpu.SemaphoreType.DMA((DIRECT,)),
                           pltpu.SemaphoreType.DMA((1,)), pltpu.VMEM((2 * units + 2, LANES), f32),
                           pltpu.SemaphoreType.DMA((4,))]),
        compiler_params=pltpu.CompilerParams(collective_id=0, has_side_effects=True, vmem_limit_bytes=VMEM_MIB * 2 ** 20),
    )(emb_grad.reshape(units, UNIT, embed), emb_param, head_grad.reshape(2, 2, 2, LANES, rows), head_param, *old)
    return results[:5], results[5:]


PIECES = 8


def apply_kernel(rows, *refs):
    (emb_dir, emb_p, emb_r, emb_c, emb_s, head_dir, head_p, head_r, head_c, head_s,
     emb_new, emb_b16, head_new, head_b16, emb_ro, emb_co, head_ro, head_co,
     emb_tmp, emb_tmp16, head_tmp, head_tmp16, sem) = refs
    size = rows // PIECES

    def piece(j, carry):
        span = pl.ds(pl.multiple_of(j * size, size), size)
        new = emb_p[span, :] - emb_dir[span, :] * emb_s[0:1, :]
        emb_tmp[span, :] = new
        emb_tmp16[span, :] = new.astype(jnp.bfloat16)
        pltpu.make_async_copy(emb_tmp.at[span], emb_new.at[span], sem.at[0]).start()
        pltpu.make_async_copy(emb_tmp16.at[span], emb_b16.at[span], sem.at[1]).start()
        for i in range(size // LANES):
            cols = pl.ds(pl.multiple_of(j * size + i * LANES, LANES), LANES)
            new = head_p[:, cols] - head_dir[:, cols] * head_s[...]
            head_tmp[:, cols] = new
            head_tmp16[:, cols] = new.astype(jnp.bfloat16)
        pltpu.make_async_copy(head_tmp.at[:, span], head_new.at[:, span], sem.at[2]).start()
        pltpu.make_async_copy(head_tmp16.at[:, span], head_b16.at[:, span], sem.at[3]).start()
        return carry

    emb_ro[...] = emb_r[...]
    emb_co[...] = emb_c[...]
    head_ro[...] = head_r[...]
    head_co[...] = head_c[...]
    lax.fori_loop(0, PIECES, piece, 0)
    arrived(emb_new, sem.at[0])
    arrived(emb_b16, sem.at[1])
    arrived(head_new, sem.at[2])
    arrived(head_b16, sem.at[3])


def apply_update(emb, head):
    rows = emb[0].shape[0]
    f32, b16 = jnp.float32, jnp.bfloat16
    hbm = pl.BlockSpec(memory_space=pltpu.HBM)
    vmem = pl.BlockSpec(memory_space=pltpu.VMEM)
    shapes = ((rows, LANES), f32), ((rows, LANES), b16), ((LANES, rows), f32), ((LANES, rows), b16)
    small = ((rows // LANES, LANES), f32), ((1, LANES), f32)
    emb_new, emb_b16, head_new, head_b16, emb_r, emb_c, head_r, head_c = pl.pallas_call(
        functools.partial(apply_kernel, rows),
        out_shape=[jax.ShapeDtypeStruct(s, t) for s, t in shapes + small + small],
        in_specs=[vmem] * 10,
        out_specs=[hbm] * 4 + [vmem] * 4,
        scratch_shapes=[pltpu.VMEM(s, t) for s, t in shapes] + [pltpu.SemaphoreType.DMA((4,))],
        compiler_params=pltpu.CompilerParams(vmem_limit_bytes=24 * 2 ** 20),
    )(*emb, *head)
    return (emb_new, head_new, emb_r.reshape(rows), emb_c.reshape(LANES), head_r.reshape(rows), head_c.reshape(LANES),
            emb_b16, head_b16)


def solution(mesh):
    arg_specs = (P("model", "data"), P("data", "model"), P("data", "model", None), P("data", None, "model"),
                 P("model"), P("data"), P("model"), P("data"))
    result_specs = (P("model", "data"), P("data", "model"), P("model"), P("data"), P("model"), P("data"),
                    P("model", "data"), P("data", "model"))

    def local_step(emb_block, head_block, emb_contrib, head_contrib, emb_rows, emb_cols, head_rows, head_cols):
        emb, head = statistics(mesh, emb_contrib[0], head_contrib[0], emb_block, head_block,
                               emb_rows, emb_cols, head_rows, head_cols)
        return apply_update(emb, head)

    return jax.shard_map(local_step, mesh=mesh, in_specs=arg_specs, out_specs=result_specs, check_vma=False)
```

```python
import functools

import jax
import jax.numpy as jnp
from jax import lax
from jax.experimental import pallas as pl
from jax.experimental.pallas import tpu as pltpu
from jax.sharding import PartitionSpec as P

TRAIN_STEP = 10
DECAY_EXP = 0.8
EPS_ONE = 1e-30
CLIP_LIMIT = 1.0
SCALE_FLOOR = 1e-3
LEARN_RATE = float(TRAIN_STEP) ** -0.5
BETA_TWO = 1.0 - float(TRAIN_STEP) ** -DECAY_EXP

MESH = pl.DeviceIdType.MESH
UNIT = 128
BIG = 4
EMB_SMALLS = 4
HEAD_SMALLS = 8
DIRECT = 4
AHEAD = 4
LAGS = (2, 4, 5, 7, 9)
LANES = 128
VMEM_KIB = 47616
PSTART = 4


class Table:
    def __init__(self, is_emb, units, grad, param, outs, bufs, small, sems, held=None):
        self.is_emb, self.grad, self.param = is_emb, grad, param
        self.smalls = EMB_SMALLS if is_emb else HEAD_SMALLS
        self.bigs = (units - self.smalls) // BIG
        self.chunks = self.smalls + self.bigs
        self.hops = self.chunks if is_emb else self.chunks - DIRECT
        self.hop_units = min(self.hops, self.bigs) * BIG + max(self.hops - self.bigs, 0)
        if is_emb:
            self.dirn, self.b16, self.row_new, self.col_new = outs
            self.pcopy, self.scale = held
        else:
            self.dirn, self.pcopy, self.row_new, self.col_new, self.scale = outs
        self.own, self.half, self.first_x, self.first_y, self.second_x, self.second_y = bufs
        (self.rpart, self.rrecv, self.rsum, self.rall, self.col_acc, self.w_acc, self.r_acc, self.p_acc, self.colx, self.scalx,
         self.vec) = small
        (self.ld, self.ra, self.rfx, self.rfy, self.rgx, self.rgy, self.rr0, self.rr1, self.rr2, self.snd, self.one) = sems
        self.rr = (self.rr0, self.rr1, self.rr2)

    def span(self, k):
        if self.is_emb:
            small = k < self.smalls
            return jnp.where(small, k, self.smalls + (k - self.smalls) * BIG), small
        small = k >= self.bigs
        return jnp.where(small, self.bigs * BIG + k - self.bigs, k * BIG), small

    def sized(self, k, act, when=True):
        first, small = self.span(k)

        @pl.when(small & when)
        def _():
            act(first, 1)

        @pl.when(jnp.logical_not(small) & when)
        def _():
            act(first, BIG)

    def units(self, k, act):
        first, small = self.span(k)

        def one(j, carry):
            act(first + j)
            return carry

        lax.fori_loop(0, jnp.where(small, 1, BIG), one, 0)


N_BUF, N_SMALL, N_SEM = 6, 11, 11
HALF = UNIT // 2


def arrived(ref, sem):
    pltpu.make_async_copy(ref, ref, sem).wait()


def lane_sum(a):
    return jnp.sum(a, axis=1, keepdims=True)


def fold8(a):
    return jnp.sum(a.reshape(a.shape[0] // 8, 8, a.shape[1]), axis=0)


def adafactor_kernel(units, nz, nd, *refs):
    emb_in, head_in, old_in = refs[0:2], refs[2:4], refs[4:8]
    pos = 8
    emb_out, head_out = refs[pos:pos + 4], refs[pos + 4:pos + 9]
    pos += 9
    emb_buf, head_buf = refs[pos:pos + N_BUF], refs[pos + N_BUF:pos + 2 * N_BUF]
    pos += 2 * N_BUF
    emb_small, head_small = refs[pos:pos + N_SMALL], refs[pos + N_SMALL:pos + 2 * N_SMALL]
    pos += 2 * N_SMALL
    emb_sem, head_sem = refs[pos:pos + N_SEM], refs[pos + N_SEM:pos + 2 * N_SEM]
    token, rall_sem, rall_snd, old, old_sem, *held = refs[pos + 2 * N_SEM:]
    emb = Table(True, units, *emb_in, emb_out, emb_buf, emb_small, emb_sem, held)
    head = Table(False, units, *head_in, head_out, head_buf, head_small, head_sem)
    vocab, embed = float(nz * units * UNIT), float(nd * LANES)
    others = nz * nd - 1
    old_rows = (0, units), (units, units), (2 * units, 1), (2 * units + 1, 1)
    hop_units = head.hop_units
    chunks = emb.chunks
    total = emb.chunks + head.chunks

    z = lax.axis_index("model")
    d = lax.axis_index("data")
    me = z * nd + d
    c = lax.rem(d, 2)
    x = lax.rem(d // 2, 2)
    y = d // 4
    partner = (z, d + 1 - 2 * c)
    xnbr = (z, d + 2 - 4 * x)
    ynbr = (z, d + 4 - 8 * y)
    ring = (partner, xnbr, ynbr)

    def send(src, dst, ssem, rsem, to):
        pltpu.make_async_remote_copy(src_ref=src, dst_ref=dst, send_sem=ssem, recv_sem=rsem,
                                     device_id=to, device_id_type=MESH).start()

    def blocks(t, u, n, core, buf):
        if t.is_emb:
            for yy in range(2):
                for xx in range(2):
                    col = pl.multiple_of(((yy * 2 + xx) * 2 + core) * LANES, LANES)
                    yield t.grad.at[pl.ds(u, n), :, pl.ds(col, LANES)], buf.at[pl.ds(u, n), yy, xx]
        else:
            for j in range(n):
                lanes = pl.ds(pl.multiple_of((u + j) * UNIT, UNIT), UNIT)
                yield t.grad.at[:, :, core, :, lanes], buf.at[u + j]

    def load(k, t):
        def act(u, n):
            for src, dst in blocks(t, u, n, c, t.own):
                pltpu.make_async_copy(src, dst, t.ld.at[k]).start()
        t.sized(k, act)

    def exchange(k, t):
        def act(u, n):
            for src, dst in blocks(t, u, n, 1 - c, t.half):
                send(src, dst, t.snd.at[0], t.ra.at[k], partner)
        t.sized(k, act)

    def first_hop(k, t):
        def act(u, n):
            part = pl.ds(u, n)
            arrived(t.own.at[part], t.ld.at[k])
            arrived(t.half.at[part], t.ra.at[k])
            for j in range(n):
                for yy in range(2):
                    t.own[u + j, yy, 1 - x, :HALF] += t.half[u + j, yy, 1 - x, :HALF]
            send(t.own.at[part, :, 1 - x, pl.ds(0, HALF)], t.first_x.at[part], t.snd.at[1], t.rfx.at[k], xnbr)
            for j in range(n):
                for xx in range(2):
                    t.own[u + j, 1 - y, xx, HALF:] += t.half[u + j, 1 - y, xx, HALF:]
            send(t.own.at[part, 1 - y, :, pl.ds(HALF, HALF)], t.first_y.at[part], t.snd.at[2], t.rfy.at[k], ynbr)
        t.sized(k, act)

    def second_hop(k, t):
        def act(u, n):
            part = pl.ds(u, n)
            arrived(t.first_x.at[part], t.rfx.at[k])
            for j in range(n):
                t.own[u + j, 1 - y, x, :HALF] += t.half[u + j, 1 - y, x, :HALF] + t.first_x[u + j, 1 - y]
            send(t.own.at[part, 1 - y, x, pl.ds(0, HALF)], t.second_x.at[part], t.snd.at[3], t.rgx.at[k], ynbr)
            arrived(t.first_y.at[part], t.rfy.at[k])
            for j in range(n):
                t.own[u + j, y, 1 - x, HALF:] += t.half[u + j, y, 1 - x, HALF:] + t.first_y[u + j, 1 - x]
            send(t.own.at[part, y, 1 - x, pl.ds(HALF, HALF)], t.second_y.at[part], t.snd.at[4], t.rgy.at[k], xnbr)
        t.sized(k, act)

    def tile(u):
        return pl.ds(pl.multiple_of(u * UNIT, UNIT), UNIT)

    def finish(k, t):
        def landed(u, n):
            arrived(t.second_x.at[pl.ds(u, n)], t.rgx.at[k])
            arrived(t.second_y.at[pl.ds(u, n)], t.rgy.at[k])

        def one(u):
            first = t.own[u, y, x, :HALF] + t.half[u, y, x, :HALF] + t.first_x[u, y] + t.second_x[u]
            last = t.own[u, y, x, HALF:] + t.half[u, y, x, HALF:] + t.first_y[u, x] + t.second_y[u]
            sq_first = first * first + EPS_ONE
            sq_last = last * last + EPS_ONE
            if t.is_emb:
                t.dirn[pl.ds(pl.multiple_of(u * UNIT, HALF), HALF), :] = first
                t.dirn[pl.ds(pl.multiple_of(u * UNIT + HALF, HALF), HALF), :] = last
                t.col_acc[...] += fold8(sq_first) + fold8(sq_last)
                sq = jnp.transpose(jnp.concatenate([sq_first, sq_last], axis=0))
                t.rpart[0, u] = jnp.sum(fold8(sq), axis=0, keepdims=True)
            else:
                t.dirn[:HALF, tile(u)] = first
                t.dirn[HALF:, tile(u)] = last
                t.col_acc[:HALF] += sq_first
                t.col_acc[HALF:] += sq_last
                t.rpart[0, u] = jnp.sum(fold8(sq_first) + fold8(sq_last), axis=0, keepdims=True)

        def pass_on(u, n):
            send(t.rpart.at[0, pl.ds(u, n)], t.rrecv.at[0, pl.ds(u, n)], t.snd.at[5], t.rr[0].at[k], ring[0])

        def to_all(u, n):
            for o in range(1, nd):
                send(t.rpart.at[0, pl.ds(u, n)], t.rall.at[d, pl.ds(u - hop_units, n)], rall_snd.at[0],
                     rall_sem.at[k - t.hops], (z, lax.rem(d + o, nd)))

        t.sized(k, landed)
        t.units(k, one)
        t.sized(k, pass_on, k < t.hops)
        if not t.is_emb:
            @pl.when(k == t.chunks - 1)
            def _():
                send_cols(t)

            t.sized(k, to_all, k >= t.hops)

    def row_hop(s, k, t):
        def act(u, n):
            part = pl.ds(u, n)
            arrived(t.rrecv.at[s - 1, part], t.rr[s - 1].at[k])
            t.rpart[s, part] = t.rpart[s - 1, part] + t.rrecv[s - 1, part]
            send(t.rpart.at[s, part], t.rrecv.at[s, part], t.snd.at[5 + s], t.rr[s].at[k], ring[s])
        t.sized(k, act, k < t.hops)

    def complete(k, t):
        def landed(u, n):
            part = pl.ds(u, n)
            arrived(t.rrecv.at[2, part], t.rr[2].at[k])
            t.rsum[part] = t.rpart[2, part] + t.rrecv[2, part]

        def landed_all(u, n):
            part = pl.ds(u - hop_units, n)
            arrived(t.rall.at[pl.ds(0, nd - 1), part], rall_sem.at[k - t.hops])
            t.rall[d, part] = t.rpart[0, pl.ds(u, n)]
            t.rsum[pl.ds(u, n)] = jnp.sum(t.rall[:, part], axis=0)

        def one(u):
            row = u if t.is_emb else units + u
            new = BETA_TWO * old[pl.ds(row, 1), :] + (1.0 - BETA_TWO) * (t.rsum[u] / embed)
            t.row_new[pl.ds(u, 1), :] = new
            t.r_acc[...] += new
            line = jnp.broadcast_to(lax.rsqrt(new), (LANES, LANES))
            if t.is_emb:
                n = t.dirn[tile(u), :] * jnp.transpose(line)
                t.dirn[tile(u), :] = n
                t.w_acc[...] += fold8(n * n)
                p = t.pcopy[tile(u), :]
            else:
                n = t.dirn[:, tile(u)] * line
                t.dirn[:, tile(u)] = n
                t.w_acc[...] += n * n
                p = t.pcopy[:, tile(u)]
            t.p_acc[...] += fold8(p * p)

        t.sized(k, landed, k < t.hops)
        if not t.is_emb:
            t.sized(k, landed_all, k >= t.hops)
        t.units(k, one)

    def per_col(t, acc):
        a = acc[...]
        return jnp.sum(a if t.is_emb else jnp.transpose(a), axis=0, keepdims=True)

    def send_cols(t):
        t.vec[0] = per_col(t, t.col_acc)
        for o in range(1, nz):
            send(t.vec.at[0], t.colx.at[z], t.one.at[0], t.one.at[1], (lax.rem(z + o, nz), d))

    def send_scalars(t):
        per_col_w = per_col(t, t.w_acc)
        r = lane_sum(t.r_acc[...]) / nd
        p = lane_sum(jnp.sum(t.p_acc[...], axis=0, keepdims=True))
        lane = lax.broadcasted_iota(jnp.int32, (1, LANES), 1)
        rest = jnp.where(lane == 1, r, jnp.where(lane == 2, p, 0.0))
        at = 2 * units + (0 if t.is_emb else 1)
        kept = BETA_TWO * old[at:at + 1, :]
        arrived(t.colx.at[pl.ds(0, nz - 1)], t.one.at[1])
        t.colx[z] = t.vec[0]
        col_sq = t.colx[0]
        for i in range(1, nz):
            col_sq = col_sq + t.colx[i]
        new = kept + (1.0 - BETA_TWO) * (col_sq / vocab)
        t.col_new[...] = new
        t.vec[1] = jnp.where(lane == 0, lane_sum(per_col_w / new), rest)
        for far in range(nz):
            plane = jnp.where(z < nz // 2, nz - 1 - far, far)
            for o in range(1, nd):
                send(t.vec.at[1], t.scalx.at[me], t.one.at[2], t.one.at[3], (plane, lax.rem(d + o, nd)))

            @pl.when(plane != z)
            def _():
                send(t.vec.at[1], t.scalx.at[me], t.one.at[2], t.one.at[3], (plane, d))

    def finish_scalars(t):
        line = lax.rsqrt(t.col_new[...])
        if t.is_emb:
            t.scale[...] = line
        else:
            t.scale[...] = jnp.transpose(jnp.broadcast_to(line, (LANES, LANES)))
        arrived(t.scalx.at[pl.ds(0, others)], t.one.at[3])
        t.scalx[me] = t.vec[1]
        total = jnp.sum(t.scalx[...], axis=0)
        lane = lax.broadcasted_iota(jnp.int32, (1, LANES), 1)
        w, r, p = (lane_sum(jnp.where(lane == i, total, 0.0)) for i in range(3))
        row_mean = r / vocab
        update_rms = jnp.sqrt(w * row_mean / (vocab * embed))
        param_rms = jnp.sqrt(p / (vocab * embed))
        step_size = LEARN_RATE * jnp.maximum(SCALE_FLOOR, param_rms) / jnp.maximum(1.0, update_rms / CLIP_LIMIT)
        t.scale[...] = t.scale[...] * (jnp.sqrt(row_mean) * step_size)

    def update_emb():
        def one(u, carry):
            new = emb.pcopy[tile(u), :] - emb.dirn[tile(u), :] * emb.scale[...]
            emb.dirn[tile(u), :] = new
            emb.b16[tile(u), :] = new.astype(jnp.bfloat16)
            return carry

        lax.fori_loop(0, units, one, 0)

    barrier = pltpu.get_barrier_semaphore()
    above, below = (lax.rem(z + 1, nz), d), (lax.rem(z + nz - 1, nz), d)

    def greet(to):
        pl.semaphore_signal(barrier, inc=1, device_id=to, device_id_type=MESH)

    for peer in ring:
        greet(peer)

    @pl.when(z < nz - 1)
    def _():
        greet(above)

    @pl.when(z > 0)
    def _():
        greet(below)

    for k in range(AHEAD):
        load(k, emb)
    for t in (emb, head):
        for acc in (t.col_acc, t.w_acc, t.r_acc, t.p_acc):
            acc[...] = jnp.zeros_like(acc)
    pl.semaphore_wait(barrier, 3 + jnp.where(z < nz - 1, 1, 0) + jnp.where(z > 0, 1, 0))

    for k in range(AHEAD):
        exchange(k, emb)

    def both(k, act):
        @pl.when((k >= 0) & (k < chunks))
        def _():
            act(k, emb)

        @pl.when((k >= chunks) & (k < total))
        def _():
            act(k - chunks, head)

    def fetch(k, t):
        load(k, t)
        exchange(k, t)

    def relay(r):
        for turn, source, last, to, sem in ((z, 0, nz - 1, above, token.at[0]), (nz - 1 - z, nz - 1, 0, below, token.at[1])):
            @pl.when(r == turn)
            def _():
                @pl.when(z != source)
                def _():
                    pl.semaphore_wait(sem, 1)

                @pl.when(z != last)
                def _():
                    pl.semaphore_signal(sem, inc=1, device_id=to, device_id_type=MESH)

    known = max(chunks - 1 + LAGS[1], LAGS[4] + 1 + nz)

    def step(i, carry):
        both(i + AHEAD, fetch)
        both(i, first_hop)

        @pl.when(i == PSTART)
        def _():
            for t in (emb, head):
                pltpu.make_async_copy(t.param, t.pcopy, t.one.at[4]).start()
            for i, (first, n) in enumerate(old_rows):
                pltpu.make_async_copy(old_in[i], old.at[pl.ds(first, n)], old_sem.at[i]).start()

        both(i - LAGS[0], second_hop)

        @pl.when(i == LAGS[4] - 1)
        def _():
            for t in (emb, head):
                arrived(t.pcopy, t.one.at[4])
            for i, (first, n) in enumerate(old_rows):
                arrived(old.at[pl.ds(first, n)], old_sem.at[i])

        both(i - LAGS[1], finish)
        relay(i - LAGS[4] - 1)

        @pl.when(i == known)
        def _():
            send_cols(emb)

        both(i - LAGS[2], functools.partial(row_hop, 1))
        both(i - LAGS[3], functools.partial(row_hop, 2))
        both(i - LAGS[4], complete)

        @pl.when(i == total + 2)
        def _():
            send_scalars(emb)

        return carry

    lax.fori_loop(0, total + LAGS[4], step, 0)
    send_scalars(head)
    finish_scalars(emb)
    update_emb()
    finish_scalars(head)

    for t in (emb, head):
        arrived(t.half, t.snd.at[0])
        arrived(t.first_x, t.snd.at[1])
        arrived(t.first_y, t.snd.at[2])
        arrived(t.second_x, t.snd.at[3])
        arrived(t.second_y, t.snd.at[4])
        hopped = t.rpart if t.is_emb else t.rpart.at[:, pl.ds(0, hop_units)]
        for s in range(3):
            arrived(hopped.at[s], t.snd.at[5 + s])
        arrived(t.colx.at[pl.ds(0, nz - 1)], t.one.at[0])
        arrived(t.scalx.at[pl.ds(0, others)], t.one.at[2])
    arrived(head.rall.at[pl.ds(0, nd - 1)], rall_snd.at[0])


def statistics(mesh, emb_grad, head_grad, emb_param, head_param, emb_row, emb_col, head_row, head_col):
    rows, embed = emb_grad.shape
    units = rows // UNIT
    chunks = max(s + (units - s) // BIG for s in (EMB_SMALLS, HEAD_SMALLS))
    nz, nd = mesh.shape["model"], mesh.shape["data"]
    f32 = jnp.float32
    old = [pltpu.with_memory_space_constraint(a.reshape(a.shape[0] // LANES, LANES), pltpu.HBM)
           for a in (emb_row, head_row, emb_col, head_col)]

    buffers = [pltpu.VMEM((units, 2, 2, UNIT, LANES), f32), pltpu.VMEM((units, 2, 2, UNIT, LANES), f32),
               pltpu.VMEM((units, 2, HALF, LANES), f32), pltpu.VMEM((units, 2, HALF, LANES), f32),
               pltpu.VMEM((units, HALF, LANES), f32), pltpu.VMEM((units, HALF, LANES), f32)]

    def small(acc_rows):
        return [pltpu.VMEM((3, units, 1, LANES), f32), pltpu.VMEM((3, units, 1, LANES), f32),
                pltpu.VMEM((units, 1, LANES), f32), pltpu.VMEM((nd, min(DIRECT, HEAD_SMALLS) + max(DIRECT - HEAD_SMALLS, 0) * BIG, 1, LANES), f32),
                pltpu.VMEM((acc_rows, LANES), f32), pltpu.VMEM((acc_rows, LANES), f32),
                pltpu.VMEM((1, LANES), f32), pltpu.VMEM((8, LANES), f32),
                pltpu.VMEM((nz, 1, LANES), f32), pltpu.VMEM((nz * nd, 1, LANES), f32), pltpu.VMEM((2, 1, LANES), f32)]

    sems = [pltpu.SemaphoreType.DMA((chunks,)) for _ in range(9)]
    sems += [pltpu.SemaphoreType.DMA((8,)), pltpu.SemaphoreType.DMA((5,))]

    stats = [jax.ShapeDtypeStruct((units, LANES), f32), jax.ShapeDtypeStruct((1, LANES), f32)]
    emb_outs = [jax.ShapeDtypeStruct((rows, LANES), f32), jax.ShapeDtypeStruct((rows, LANES), jnp.bfloat16)] + stats
    head_outs = [jax.ShapeDtypeStruct((LANES, rows), f32)] * 2 + stats + [jax.ShapeDtypeStruct((LANES, LANES), f32)]
    hbm = pl.BlockSpec(memory_space=pltpu.HBM)
    vmem = pl.BlockSpec(memory_space=pltpu.VMEM)
    results = pl.pallas_call(
        functools.partial(adafactor_kernel, units, nz, nd),
        out_shape=emb_outs + head_outs,
        in_specs=[hbm] * 8,
        out_specs=[vmem] * 9,
        scratch_shapes=(buffers + buffers + small(8) + small(LANES) + sems + sems
                        + [pltpu.SemaphoreType.REGULAR((2,)), pltpu.SemaphoreType.DMA((DIRECT,)),
                           pltpu.SemaphoreType.DMA((1,)), pltpu.VMEM((2 * units + 2, LANES), f32),
                           pltpu.SemaphoreType.DMA((4,)), pltpu.VMEM((rows, LANES), f32), pltpu.VMEM((1, LANES), f32)]),
        compiler_params=pltpu.CompilerParams(collective_id=0, has_side_effects=True, vmem_limit_bytes=VMEM_KIB * 1024),
    )(emb_grad.reshape(units, UNIT, embed), emb_param, head_grad.reshape(2, 2, 2, LANES, rows), head_param, *old)
    return results


PIECES = 8


def apply_kernel(rows, *refs):
    ready, (head_dir, head_p, head_r, head_c, head_s) = refs[:4], refs[4:9]
    out, (head_new, head_b16, head_ro, head_co) = refs[9:13], refs[13:17]
    head_tmp, head_tmp16, sem = refs[17:]
    for i, (src, dst) in enumerate(zip(ready + (head_r, head_c), out + (head_ro, head_co))):
        pltpu.make_async_copy(src, dst, sem.at[2 + i]).start()
    size = rows // PIECES

    def piece(j, carry):
        span = pl.ds(pl.multiple_of(j * size, size), size)
        for i in range(size // LANES):
            cols = pl.ds(pl.multiple_of(j * size + i * LANES, LANES), LANES)
            new = head_p[:, cols] - head_dir[:, cols] * head_s[...]
            head_tmp[:, cols] = new
            head_tmp16[:, cols] = new.astype(jnp.bfloat16)
        pltpu.make_async_copy(head_tmp.at[:, span], head_new.at[:, span], sem.at[0]).start()
        pltpu.make_async_copy(head_tmp16.at[:, span], head_b16.at[:, span], sem.at[1]).start()
        return carry

    lax.fori_loop(0, PIECES, piece, 0)
    arrived(head_new, sem.at[0])
    arrived(head_b16, sem.at[1])
    for i, dst in enumerate(out + (head_ro, head_co)):
        arrived(dst, sem.at[2 + i])


def apply_update(results):
    rows = results[0].shape[0]
    f32, b16 = jnp.float32, jnp.bfloat16
    hbm = pl.BlockSpec(memory_space=pltpu.HBM)
    vmem = pl.BlockSpec(memory_space=pltpu.VMEM)
    stats = ((rows // LANES, LANES), f32), ((1, LANES), f32)
    shapes = (((rows, LANES), f32), ((rows, LANES), b16)) + stats + (((LANES, rows), f32), ((LANES, rows), b16)) + stats
    emb_new, emb_b16, emb_r, emb_c, head_new, head_b16, head_r, head_c = pl.pallas_call(
        functools.partial(apply_kernel, rows),
        out_shape=[jax.ShapeDtypeStruct(s, t) for s, t in shapes],
        in_specs=[vmem] * 9,
        out_specs=[hbm] * 8,
        scratch_shapes=[pltpu.VMEM((LANES, rows), f32), pltpu.VMEM((LANES, rows), b16), pltpu.SemaphoreType.DMA((8,))],
        compiler_params=pltpu.CompilerParams(vmem_limit_bytes=24 * 2 ** 20),
    )(*results)
    return (emb_new, head_new, emb_r.reshape(rows), emb_c.reshape(LANES), head_r.reshape(rows), head_c.reshape(LANES),
            emb_b16, head_b16)


def solution(mesh):
    arg_specs = (P("model", "data"), P("data", "model"), P("data", "model", None), P("data", None, "model"),
                 P("model"), P("data"), P("model"), P("data"))
    result_specs = (P("model", "data"), P("data", "model"), P("model"), P("data"), P("model"), P("data"),
                    P("model", "data"), P("data", "model"))

    def local_step(emb_block, head_block, emb_contrib, head_contrib, emb_rows, emb_cols, head_rows, head_cols):
        return apply_update(statistics(mesh, emb_contrib[0], head_contrib[0], emb_block, head_block,
                                       emb_rows, emb_cols, head_rows, head_cols))

    return jax.shard_map(local_step, mesh=mesh, in_specs=arg_specs, out_specs=result_specs, check_vma=False)
```

```python
import functools

import jax
import jax.numpy as jnp
from jax import lax
from jax.experimental import pallas as pl
from jax.experimental.pallas import tpu as pltpu
from jax.sharding import PartitionSpec as P

TRAIN_STEP = 10
DECAY_EXP = 0.8
EPS_ONE = 1e-30
CLIP_LIMIT = 1.0
SCALE_FLOOR = 1e-3
LEARN_RATE = float(TRAIN_STEP) ** -0.5
BETA_TWO = 1.0 - float(TRAIN_STEP) ** -DECAY_EXP

MESH = pl.DeviceIdType.MESH
UNIT = 128
BIG = 4
EMB_SMALLS = 4
HEAD_SMALLS = 4
DIRECT = 4
AHEAD = 4
LAGS = (2, 4, 5, 7, 9)
LANES = 128
VMEM_KIB = 47616
PSTART = 4


class Table:
    def __init__(self, is_emb, units, grad, param, outs, bufs, small, sems, held=None):
        self.is_emb, self.grad, self.param = is_emb, grad, param
        self.smalls = EMB_SMALLS if is_emb else HEAD_SMALLS
        self.bigs = (units - self.smalls) // BIG
        self.chunks = self.smalls + self.bigs
        self.hops = self.chunks if is_emb else self.chunks - DIRECT
        self.hop_units = min(self.hops, self.bigs) * BIG + max(self.hops - self.bigs, 0)
        if is_emb:
            self.dirn, self.b16, self.row_new, self.col_new = outs
            self.pcopy, self.scale = held
        else:
            self.dirn, self.pcopy, self.row_new, self.col_new, self.scale = outs
        self.own, self.half, self.first_x, self.first_y, self.second_x, self.second_y = bufs
        (self.rpart, self.rrecv, self.rsum, self.rall, self.col_acc, self.w_acc, self.r_acc, self.p_acc, self.colx, self.scalx,
         self.vec) = small
        (self.ld, self.ra, self.rfx, self.rfy, self.rgx, self.rgy, self.rr0, self.rr1, self.rr2, self.snd, self.one) = sems
        self.rr = (self.rr0, self.rr1, self.rr2)

    def span(self, k):
        if self.is_emb:
            small = k < self.smalls
            return jnp.where(small, k, self.smalls + (k - self.smalls) * BIG), small
        small = k >= self.bigs
        return jnp.where(small, self.bigs * BIG + k - self.bigs, k * BIG), small

    def sized(self, k, act, when=True):
        first, small = self.span(k)

        @pl.when(small & when)
        def _():
            act(first, 1)

        @pl.when(jnp.logical_not(small) & when)
        def _():
            act(first, BIG)

    def units(self, k, act):
        first, small = self.span(k)

        def one(j, carry):
            act(first + j)
            return carry

        lax.fori_loop(0, jnp.where(small, 1, BIG), one, 0)


N_BUF, N_SMALL, N_SEM = 6, 11, 11
HALF = UNIT // 2


def arrived(ref, sem):
    pltpu.make_async_copy(ref, ref, sem).wait()


def lane_sum(a):
    return jnp.sum(a, axis=1, keepdims=True)


def fold8(a):
    return jnp.sum(a.reshape(a.shape[0] // 8, 8, a.shape[1]), axis=0)


def adafactor_kernel(units, nz, nd, *refs):
    emb_in, head_in, old_in = refs[0:2], refs[2:4], refs[4:8]
    pos = 8
    emb_out, head_out = refs[pos:pos + 4], refs[pos + 4:pos + 9]
    pos += 9
    emb_buf, head_buf = refs[pos:pos + N_BUF], refs[pos + N_BUF:pos + 2 * N_BUF]
    pos += 2 * N_BUF
    emb_small, head_small = refs[pos:pos + N_SMALL], refs[pos + N_SMALL:pos + 2 * N_SMALL]
    pos += 2 * N_SMALL
    emb_sem, head_sem = refs[pos:pos + N_SEM], refs[pos + N_SEM:pos + 2 * N_SEM]
    token, rall_sem, rall_snd, old, old_sem, *held = refs[pos + 2 * N_SEM:]
    emb = Table(True, units, *emb_in, emb_out, emb_buf, emb_small, emb_sem, held)
    head = Table(False, units, *head_in, head_out, head_buf, head_small, head_sem)
    vocab, embed = float(nz * units * UNIT), float(nd * LANES)
    others = nz * nd - 1
    old_rows = (0, units), (units, units), (2 * units, 1), (2 * units + 1, 1)
    hop_units = head.hop_units
    chunks = emb.chunks
    total = emb.chunks + head.chunks

    z = lax.axis_index("model")
    d = lax.axis_index("data")
    me = z * nd + d
    c = lax.rem(d, 2)
    x = lax.rem(d // 2, 2)
    y = d // 4
    partner = (z, d + 1 - 2 * c)
    xnbr = (z, d + 2 - 4 * x)
    ynbr = (z, d + 4 - 8 * y)
    ring = (partner, xnbr, ynbr)

    def send(src, dst, ssem, rsem, to):
        pltpu.make_async_remote_copy(src_ref=src, dst_ref=dst, send_sem=ssem, recv_sem=rsem,
                                     device_id=to, device_id_type=MESH).start()

    def blocks(t, u, n, core, buf):
        if t.is_emb:
            for yy in range(2):
                for xx in range(2):
                    col = pl.multiple_of(((yy * 2 + xx) * 2 + core) * LANES, LANES)
                    yield t.grad.at[pl.ds(u, n), :, pl.ds(col, LANES)], buf.at[pl.ds(u, n), yy, xx]
        else:
            for j in range(n):
                lanes = pl.ds(pl.multiple_of((u + j) * UNIT, UNIT), UNIT)
                yield t.grad.at[:, :, core, :, lanes], buf.at[u + j]

    def load(k, t):
        def act(u, n):
            for src, dst in blocks(t, u, n, c, t.own):
                pltpu.make_async_copy(src, dst, t.ld.at[k]).start()
        t.sized(k, act)

    def exchange(k, t):
        def act(u, n):
            for src, dst in blocks(t, u, n, 1 - c, t.half):
                send(src, dst, t.snd.at[0], t.ra.at[k], partner)
        t.sized(k, act)

    def first_hop(k, t):
        def act(u, n):
            part = pl.ds(u, n)
            arrived(t.own.at[part], t.ld.at[k])
            arrived(t.half.at[part], t.ra.at[k])
            for j in range(n):
                for yy in range(2):
                    t.own[u + j, yy, 1 - x, :HALF] += t.half[u + j, yy, 1 - x, :HALF]
            send(t.own.at[part, :, 1 - x, pl.ds(0, HALF)], t.first_x.at[part], t.snd.at[1], t.rfx.at[k], xnbr)
            for j in range(n):
                for xx in range(2):
                    t.own[u + j, 1 - y, xx, HALF:] += t.half[u + j, 1 - y, xx, HALF:]
            send(t.own.at[part, 1 - y, :, pl.ds(HALF, HALF)], t.first_y.at[part], t.snd.at[2], t.rfy.at[k], ynbr)
        t.sized(k, act)

    def second_hop(k, t):
        def act(u, n):
            part = pl.ds(u, n)
            arrived(t.first_x.at[part], t.rfx.at[k])
            for j in range(n):
                t.own[u + j, 1 - y, x, :HALF] += t.half[u + j, 1 - y, x, :HALF] + t.first_x[u + j, 1 - y]
            send(t.own.at[part, 1 - y, x, pl.ds(0, HALF)], t.second_x.at[part], t.snd.at[3], t.rgx.at[k], ynbr)
            arrived(t.first_y.at[part], t.rfy.at[k])
            for j in range(n):
                t.own[u + j, y, 1 - x, HALF:] += t.half[u + j, y, 1 - x, HALF:] + t.first_y[u + j, 1 - x]
            send(t.own.at[part, y, 1 - x, pl.ds(HALF, HALF)], t.second_y.at[part], t.snd.at[4], t.rgy.at[k], xnbr)
        t.sized(k, act)

    def tile(u):
        return pl.ds(pl.multiple_of(u * UNIT, UNIT), UNIT)

    def finish(k, t):
        def landed(u, n):
            arrived(t.second_x.at[pl.ds(u, n)], t.rgx.at[k])
            arrived(t.second_y.at[pl.ds(u, n)], t.rgy.at[k])

        def one(u):
            first = t.own[u, y, x, :HALF] + t.half[u, y, x, :HALF] + t.first_x[u, y] + t.second_x[u]
            last = t.own[u, y, x, HALF:] + t.half[u, y, x, HALF:] + t.first_y[u, x] + t.second_y[u]
            sq_first = first * first + EPS_ONE
            sq_last = last * last + EPS_ONE
            if t.is_emb:
                t.dirn[pl.ds(pl.multiple_of(u * UNIT, HALF), HALF), :] = first
                t.dirn[pl.ds(pl.multiple_of(u * UNIT + HALF, HALF), HALF), :] = last
                t.col_acc[...] += fold8(sq_first) + fold8(sq_last)
                sq = jnp.transpose(jnp.concatenate([sq_first, sq_last], axis=0))
                t.rpart[0, u] = jnp.sum(fold8(sq), axis=0, keepdims=True)
            else:
                t.dirn[:HALF, tile(u)] = first
                t.dirn[HALF:, tile(u)] = last
                t.col_acc[:HALF] += sq_first
                t.col_acc[HALF:] += sq_last
                t.rpart[0, u] = jnp.sum(fold8(sq_first) + fold8(sq_last), axis=0, keepdims=True)

        def pass_on(u, n):
            send(t.rpart.at[0, pl.ds(u, n)], t.rrecv.at[0, pl.ds(u, n)], t.snd.at[5], t.rr[0].at[k], ring[0])

        def to_all(u, n):
            for o in range(1, nd):
                send(t.rpart.at[0, pl.ds(u, n)], t.rall.at[d, pl.ds(u - hop_units, n)], rall_snd.at[0],
                     rall_sem.at[k - t.hops], (z, lax.rem(d + o, nd)))

        t.sized(k, landed)
        t.units(k, one)
        t.sized(k, pass_on, k < t.hops)
        if not t.is_emb:
            @pl.when(k == t.chunks - 1)
            def _():
                send_cols(t)

            t.sized(k, to_all, k >= t.hops)

    def row_hop(s, k, t):
        def act(u, n):
            part = pl.ds(u, n)
            arrived(t.rrecv.at[s - 1, part], t.rr[s - 1].at[k])
            t.rpart[s, part] = t.rpart[s - 1, part] + t.rrecv[s - 1, part]
            send(t.rpart.at[s, part], t.rrecv.at[s, part], t.snd.at[5 + s], t.rr[s].at[k], ring[s])
        t.sized(k, act, k < t.hops)

    def complete(k, t):
        def landed(u, n):
            part = pl.ds(u, n)
            arrived(t.rrecv.at[2, part], t.rr[2].at[k])
            t.rsum[part] = t.rpart[2, part] + t.rrecv[2, part]

        def landed_all(u, n):
            part = pl.ds(u - hop_units, n)
            arrived(t.rall.at[pl.ds(0, nd - 1), part], rall_sem.at[k - t.hops])
            t.rall[d, part] = t.rpart[0, pl.ds(u, n)]
            t.rsum[pl.ds(u, n)] = jnp.sum(t.rall[:, part], axis=0)

        def one(u):
            row = u if t.is_emb else units + u
            new = BETA_TWO * old[pl.ds(row, 1), :] + (1.0 - BETA_TWO) * (t.rsum[u] / embed)
            t.row_new[pl.ds(u, 1), :] = new
            t.r_acc[...] += new
            line = jnp.broadcast_to(lax.rsqrt(new), (LANES, LANES))
            if t.is_emb:
                n = t.dirn[tile(u), :] * jnp.transpose(line)
                t.dirn[tile(u), :] = n
                t.w_acc[...] += fold8(n * n)
                p = t.pcopy[tile(u), :]
            else:
                n = t.dirn[:, tile(u)] * line
                t.dirn[:, tile(u)] = n
                t.w_acc[...] += n * n
                p = t.pcopy[:, tile(u)]
            t.p_acc[...] += fold8(p * p)

        t.sized(k, landed, k < t.hops)
        if not t.is_emb:
            t.sized(k, landed_all, k >= t.hops)
        t.units(k, one)

    def per_col(t, acc):
        a = acc[...]
        return jnp.sum(a if t.is_emb else jnp.transpose(a), axis=0, keepdims=True)

    def send_cols(t):
        t.vec[0] = per_col(t, t.col_acc)
        for o in range(1, nz):
            send(t.vec.at[0], t.colx.at[z], t.one.at[0], t.one.at[1], (lax.rem(z + o, nz), d))

    def columns(t):
        at = 2 * units + (0 if t.is_emb else 1)
        kept = BETA_TWO * old[at:at + 1, :]
        arrived(t.colx.at[pl.ds(0, nz - 1)], t.one.at[1])
        t.colx[z] = t.vec[0]
        col_sq = t.colx[0]
        for i in range(1, nz):
            col_sq = col_sq + t.colx[i]
        new = kept + (1.0 - BETA_TWO) * (col_sq / vocab)
        t.col_new[...] = new
        inverse = 1.0 / new
        t.scale[...] = inverse if t.is_emb else jnp.transpose(jnp.broadcast_to(inverse, (LANES, LANES)))

    def send_scalars(t):
        w = lane_sum(jnp.sum(fold8(t.w_acc[...] * t.scale[...]), axis=0, keepdims=True))
        r = lane_sum(t.r_acc[...]) / nd
        p = lane_sum(jnp.sum(t.p_acc[...], axis=0, keepdims=True))
        lane = lax.broadcasted_iota(jnp.int32, (1, LANES), 1)
        t.vec[1] = jnp.where(lane == 0, w, jnp.where(lane == 1, r, jnp.where(lane == 2, p, 0.0)))
        for far in range(nz):
            plane = jnp.where(z < nz // 2, nz - 1 - far, far)
            for o in range(1, nd):
                send(t.vec.at[1], t.scalx.at[me], t.one.at[2], t.one.at[3], (plane, lax.rem(d + o, nd)))

            @pl.when(plane != z)
            def _():
                send(t.vec.at[1], t.scalx.at[me], t.one.at[2], t.one.at[3], (plane, d))

    def finish_scalars(t):
        line = lax.rsqrt(t.col_new[...])
        if t.is_emb:
            t.scale[...] = line
        else:
            t.scale[...] = jnp.transpose(jnp.broadcast_to(line, (LANES, LANES)))
        arrived(t.scalx.at[pl.ds(0, others)], t.one.at[3])
        t.scalx[me] = t.vec[1]
        total = jnp.sum(t.scalx[...], axis=0)
        lane = lax.broadcasted_iota(jnp.int32, (1, LANES), 1)
        w, r, p = (lane_sum(jnp.where(lane == i, total, 0.0)) for i in range(3))
        row_mean = r / vocab
        update_rms = jnp.sqrt(w * row_mean / (vocab * embed))
        param_rms = jnp.sqrt(p / (vocab * embed))
        step_size = LEARN_RATE * jnp.maximum(SCALE_FLOOR, param_rms) / jnp.maximum(1.0, update_rms / CLIP_LIMIT)
        t.scale[...] = t.scale[...] * (jnp.sqrt(row_mean) * step_size)

    def update_emb():
        def one(u, carry):
            new = emb.pcopy[tile(u), :] - emb.dirn[tile(u), :] * emb.scale[...]
            emb.dirn[tile(u), :] = new
            emb.b16[tile(u), :] = new.astype(jnp.bfloat16)
            return carry

        lax.fori_loop(0, units, one, 0)

    barrier = pltpu.get_barrier_semaphore()
    above, below = (lax.rem(z + 1, nz), d), (lax.rem(z + nz - 1, nz), d)

    def greet(to):
        pl.semaphore_signal(barrier, inc=1, device_id=to, device_id_type=MESH)

    for peer in ring:
        greet(peer)

    @pl.when(z < nz - 1)
    def _():
        greet(above)

    @pl.when(z > 0)
    def _():
        greet(below)

    for k in range(AHEAD):
        load(k, emb)
    for t in (emb, head):
        for acc in (t.col_acc, t.w_acc, t.r_acc, t.p_acc):
            acc[...] = jnp.zeros_like(acc)
    pl.semaphore_wait(barrier, 3 + jnp.where(z < nz - 1, 1, 0) + jnp.where(z > 0, 1, 0))

    for k in range(AHEAD):
        exchange(k, emb)

    def both(k, act):
        @pl.when((k >= 0) & (k < chunks))
        def _():
            act(k, emb)

        @pl.when((k >= chunks) & (k < total))
        def _():
            act(k - chunks, head)

    def fetch(k, t):
        load(k, t)
        exchange(k, t)

    def relay(r):
        for turn, source, last, to, sem in ((z, 0, nz - 1, above, token.at[0]), (nz - 1 - z, nz - 1, 0, below, token.at[1])):
            @pl.when(r == turn)
            def _():
                @pl.when(z != source)
                def _():
                    pl.semaphore_wait(sem, 1)

                @pl.when(z != last)
                def _():
                    pl.semaphore_signal(sem, inc=1, device_id=to, device_id_type=MESH)

    known = max(chunks - 1 + LAGS[1], LAGS[4] + 1 + nz)

    def step(i, carry):
        both(i + AHEAD, fetch)
        both(i, first_hop)

        @pl.when(i == PSTART)
        def _():
            for t in (emb, head):
                pltpu.make_async_copy(t.param, t.pcopy, t.one.at[4]).start()
            for i, (first, n) in enumerate(old_rows):
                pltpu.make_async_copy(old_in[i], old.at[pl.ds(first, n)], old_sem.at[i]).start()

        both(i - LAGS[0], second_hop)

        @pl.when(i == LAGS[4] - 1)
        def _():
            for t in (emb, head):
                arrived(t.pcopy, t.one.at[4])
            for i, (first, n) in enumerate(old_rows):
                arrived(old.at[pl.ds(first, n)], old_sem.at[i])

        both(i - LAGS[1], finish)
        relay(i - LAGS[4] - 1)

        @pl.when(i == known)
        def _():
            send_cols(emb)

        both(i - LAGS[2], functools.partial(row_hop, 1))
        both(i - LAGS[3], functools.partial(row_hop, 2))

        @pl.when(i == total - 1 + LAGS[4])
        def _():
            columns(head)

        both(i - LAGS[4], complete)

        @pl.when(i == total + 2)
        def _():
            columns(emb)
            send_scalars(emb)

        return carry

    lax.fori_loop(0, total + LAGS[4], step, 0)
    send_scalars(head)
    finish_scalars(emb)
    update_emb()
    finish_scalars(head)

    for t in (emb, head):
        arrived(t.half, t.snd.at[0])
        arrived(t.first_x, t.snd.at[1])
        arrived(t.first_y, t.snd.at[2])
        arrived(t.second_x, t.snd.at[3])
        arrived(t.second_y, t.snd.at[4])
        hopped = t.rpart if t.is_emb else t.rpart.at[:, pl.ds(0, hop_units)]
        for s in range(3):
            arrived(hopped.at[s], t.snd.at[5 + s])
        arrived(t.colx.at[pl.ds(0, nz - 1)], t.one.at[0])
        arrived(t.scalx.at[pl.ds(0, others)], t.one.at[2])
    arrived(head.rall.at[pl.ds(0, nd - 1)], rall_snd.at[0])


def statistics(mesh, emb_grad, head_grad, emb_param, head_param, emb_row, emb_col, head_row, head_col):
    rows, embed = emb_grad.shape
    units = rows // UNIT
    chunks = max(s + (units - s) // BIG for s in (EMB_SMALLS, HEAD_SMALLS))
    nz, nd = mesh.shape["model"], mesh.shape["data"]
    f32 = jnp.float32
    old = [pltpu.with_memory_space_constraint(a.reshape(a.shape[0] // LANES, LANES), pltpu.HBM)
           for a in (emb_row, head_row, emb_col, head_col)]

    buffers = [pltpu.VMEM((units, 2, 2, UNIT, LANES), f32), pltpu.VMEM((units, 2, 2, UNIT, LANES), f32),
               pltpu.VMEM((units, 2, HALF, LANES), f32), pltpu.VMEM((units, 2, HALF, LANES), f32),
               pltpu.VMEM((units, HALF, LANES), f32), pltpu.VMEM((units, HALF, LANES), f32)]

    def small(acc_rows):
        return [pltpu.VMEM((3, units, 1, LANES), f32), pltpu.VMEM((3, units, 1, LANES), f32),
                pltpu.VMEM((units, 1, LANES), f32), pltpu.VMEM((nd, min(DIRECT, HEAD_SMALLS) + max(DIRECT - HEAD_SMALLS, 0) * BIG, 1, LANES), f32),
                pltpu.VMEM((acc_rows, LANES), f32), pltpu.VMEM((acc_rows, LANES), f32),
                pltpu.VMEM((1, LANES), f32), pltpu.VMEM((8, LANES), f32),
                pltpu.VMEM((nz, 1, LANES), f32), pltpu.VMEM((nz * nd, 1, LANES), f32), pltpu.VMEM((2, 1, LANES), f32)]

    sems = [pltpu.SemaphoreType.DMA((chunks,)) for _ in range(9)]
    sems += [pltpu.SemaphoreType.DMA((8,)), pltpu.SemaphoreType.DMA((5,))]

    stats = [jax.ShapeDtypeStruct((units, LANES), f32), jax.ShapeDtypeStruct((1, LANES), f32)]
    emb_outs = [jax.ShapeDtypeStruct((rows, LANES), f32), jax.ShapeDtypeStruct((rows, LANES), jnp.bfloat16)] + stats
    head_outs = [jax.ShapeDtypeStruct((LANES, rows), f32)] * 2 + stats + [jax.ShapeDtypeStruct((LANES, LANES), f32)]
    hbm = pl.BlockSpec(memory_space=pltpu.HBM)
    vmem = pl.BlockSpec(memory_space=pltpu.VMEM)
    results = pl.pallas_call(
        functools.partial(adafactor_kernel, units, nz, nd),
        out_shape=emb_outs + head_outs,
        in_specs=[hbm] * 8,
        out_specs=[vmem] * 9,
        scratch_shapes=(buffers + buffers + small(8) + small(LANES) + sems + sems
                        + [pltpu.SemaphoreType.REGULAR((2,)), pltpu.SemaphoreType.DMA((DIRECT,)),
                           pltpu.SemaphoreType.DMA((1,)), pltpu.VMEM((2 * units + 2, LANES), f32),
                           pltpu.SemaphoreType.DMA((4,)), pltpu.VMEM((rows, LANES), f32), pltpu.VMEM((1, LANES), f32)]),
        compiler_params=pltpu.CompilerParams(collective_id=0, has_side_effects=True, vmem_limit_bytes=VMEM_KIB * 1024),
    )(emb_grad.reshape(units, UNIT, embed), emb_param, head_grad.reshape(2, 2, 2, LANES, rows), head_param, *old)
    return results


PIECES = 8


def apply_kernel(rows, *refs):
    ready, (head_dir, head_p, head_r, head_c, head_s) = refs[:4], refs[4:9]
    out, (head_new, head_b16, head_ro, head_co) = refs[9:13], refs[13:17]
    head_tmp, head_tmp16, sem = refs[17:]
    for i, (src, dst) in enumerate(zip(ready + (head_r, head_c), out + (head_ro, head_co))):
        pltpu.make_async_copy(src, dst, sem.at[2 + i]).start()
    size = rows // PIECES

    def piece(j, carry):
        span = pl.ds(pl.multiple_of(j * size, size), size)
        for i in range(size // LANES):
            cols = pl.ds(pl.multiple_of(j * size + i * LANES, LANES), LANES)
            new = head_p[:, cols] - head_dir[:, cols] * head_s[...]
            head_tmp[:, cols] = new
            head_tmp16[:, cols] = new.astype(jnp.bfloat16)
        pltpu.make_async_copy(head_tmp.at[:, span], head_new.at[:, span], sem.at[0]).start()
        pltpu.make_async_copy(head_tmp16.at[:, span], head_b16.at[:, span], sem.at[1]).start()
        return carry

    lax.fori_loop(0, PIECES, piece, 0)
    arrived(head_new, sem.at[0])
    arrived(head_b16, sem.at[1])
    for i, dst in enumerate(out + (head_ro, head_co)):
        arrived(dst, sem.at[2 + i])


def apply_update(results):
    rows = results[0].shape[0]
    f32, b16 = jnp.float32, jnp.bfloat16
    hbm = pl.BlockSpec(memory_space=pltpu.HBM)
    vmem = pl.BlockSpec(memory_space=pltpu.VMEM)
    stats = ((rows // LANES, LANES), f32), ((1, LANES), f32)
    shapes = (((rows, LANES), f32), ((rows, LANES), b16)) + stats + (((LANES, rows), f32), ((LANES, rows), b16)) + stats
    emb_new, emb_b16, emb_r, emb_c, head_new, head_b16, head_r, head_c = pl.pallas_call(
        functools.partial(apply_kernel, rows),
        out_shape=[jax.ShapeDtypeStruct(s, t) for s, t in shapes],
        in_specs=[vmem] * 9,
        out_specs=[hbm] * 8,
        scratch_shapes=[pltpu.VMEM((LANES, rows), f32), pltpu.VMEM((LANES, rows), b16), pltpu.SemaphoreType.DMA((8,))],
        compiler_params=pltpu.CompilerParams(vmem_limit_bytes=24 * 2 ** 20),
    )(*results)
    return (emb_new, head_new, emb_r.reshape(rows), emb_c.reshape(LANES), head_r.reshape(rows), head_c.reshape(LANES),
            emb_b16, head_b16)


def solution(mesh):
    arg_specs = (P("model", "data"), P("data", "model"), P("data", "model", None), P("data", None, "model"),
                 P("model"), P("data"), P("model"), P("data"))
    result_specs = (P("model", "data"), P("data", "model"), P("model"), P("data"), P("model"), P("data"),
                    P("model", "data"), P("data", "model"))

    def local_step(emb_block, head_block, emb_contrib, head_contrib, emb_rows, emb_cols, head_rows, head_cols):
        return apply_update(statistics(mesh, emb_contrib[0], head_contrib[0], emb_block, head_block,
                                       emb_rows, emb_cols, head_rows, head_cols))

    return jax.shard_map(local_step, mesh=mesh, in_specs=arg_specs, out_specs=result_specs, check_vma=False)
```

```python
import functools

import jax
import jax.numpy as jnp
from jax import lax
from jax.experimental import pallas as pl
from jax.experimental.pallas import tpu as pltpu
from jax.sharding import PartitionSpec as P

TRAIN_STEP = 10
DECAY_EXP = 0.8
EPS_ONE = 1e-30
CLIP_LIMIT = 1.0
SCALE_FLOOR = 1e-3
LEARN_RATE = float(TRAIN_STEP) ** -0.5
BETA_TWO = 1.0 - float(TRAIN_STEP) ** -DECAY_EXP

MESH = pl.DeviceIdType.MESH
UNIT = 128
BIG = 7
EMB_SMALLS = 4
HEAD_SMALLS = 4
DIRECT = 4
AHEAD = 4
LAGS = (2, 4, 5, 7, 9)
LANES = 128
VMEM_KIB = 47616
PSTART = 4


class Table:
    def __init__(self, is_emb, units, grad, param, outs, bufs, small, sems, held=None):
        self.is_emb, self.grad, self.param = is_emb, grad, param
        self.smalls = EMB_SMALLS if is_emb else HEAD_SMALLS
        self.bigs = (units - self.smalls) // BIG
        self.chunks = self.smalls + self.bigs
        self.hops = self.chunks if is_emb else self.chunks - DIRECT
        self.hop_units = min(self.hops, self.bigs) * BIG + max(self.hops - self.bigs, 0)
        if is_emb:
            self.dirn, self.b16, self.row_new, self.col_new = outs
            self.pcopy, self.scale = held
        else:
            self.dirn, self.pcopy, self.row_new, self.col_new, self.scale = outs
        self.own, self.half, self.first_x, self.first_y, self.second_x, self.second_y = bufs
        (self.rpart, self.rrecv, self.rsum, self.rall, self.col_acc, self.w_acc, self.r_acc, self.p_acc, self.colx, self.scalx,
         self.vec) = small
        (self.ld, self.ra, self.rfx, self.rfy, self.rgx, self.rgy, self.rr0, self.rr1, self.rr2, self.snd, self.one) = sems
        self.rr = (self.rr0, self.rr1, self.rr2)

    def span(self, k):
        if self.is_emb:
            small = k < self.smalls
            return jnp.where(small, k, self.smalls + (k - self.smalls) * BIG), small
        small = k >= self.bigs
        return jnp.where(small, self.bigs * BIG + k - self.bigs, k * BIG), small

    def sized(self, k, act, when=True):
        first, small = self.span(k)

        @pl.when(small & when)
        def _():
            act(first, 1)

        @pl.when(jnp.logical_not(small) & when)
        def _():
            act(first, BIG)

    def units(self, k, act):
        first, small = self.span(k)

        def one(j, carry):
            act(first + j)
            return carry

        lax.fori_loop(0, jnp.where(small, 1, BIG), one, 0)


N_BUF, N_SMALL, N_SEM = 6, 11, 11
HALF = UNIT // 2


def arrived(ref, sem):
    pltpu.make_async_copy(ref, ref, sem).wait()


def lane_sum(a):
    return jnp.sum(a, axis=1, keepdims=True)


def fold8(a):
    return jnp.sum(a.reshape(a.shape[0] // 8, 8, a.shape[1]), axis=0)


def adafactor_kernel(units, nz, nd, *refs):
    emb_in, head_in, old_in = refs[0:2], refs[2:4], refs[4:8]
    pos = 8
    emb_out, head_out = refs[pos:pos + 4], refs[pos + 4:pos + 9]
    pos += 9
    emb_buf, head_buf = refs[pos:pos + N_BUF], refs[pos + N_BUF:pos + 2 * N_BUF]
    pos += 2 * N_BUF
    emb_small, head_small = refs[pos:pos + N_SMALL], refs[pos + N_SMALL:pos + 2 * N_SMALL]
    pos += 2 * N_SMALL
    emb_sem, head_sem = refs[pos:pos + N_SEM], refs[pos + N_SEM:pos + 2 * N_SEM]
    token, rall_sem, rall_snd, old, old_sem, *held = refs[pos + 2 * N_SEM:]
    emb = Table(True, units, *emb_in, emb_out, emb_buf, emb_small, emb_sem, held)
    head = Table(False, units, *head_in, head_out, head_buf, head_small, head_sem)
    vocab, embed = float(nz * units * UNIT), float(nd * LANES)
    others = nz * nd - 1
    old_rows = (0, units), (units, units), (2 * units, 1), (2 * units + 1, 1)
    hop_units = head.hop_units
    chunks = emb.chunks
    total = emb.chunks + head.chunks

    z = lax.axis_index("model")
    d = lax.axis_index("data")
    me = z * nd + d
    c = lax.rem(d, 2)
    x = lax.rem(d // 2, 2)
    y = d // 4
    partner = (z, d + 1 - 2 * c)
    xnbr = (z, d + 2 - 4 * x)
    ynbr = (z, d + 4 - 8 * y)
    ring = (partner, xnbr, ynbr)

    def send(src, dst, ssem, rsem, to):
        pltpu.make_async_remote_copy(src_ref=src, dst_ref=dst, send_sem=ssem, recv_sem=rsem,
                                     device_id=to, device_id_type=MESH).start()

    def blocks(t, u, n, core, buf):
        if t.is_emb:
            for yy in range(2):
                for xx in range(2):
                    col = pl.multiple_of(((yy * 2 + xx) * 2 + core) * LANES, LANES)
                    yield t.grad.at[pl.ds(u, n), :, pl.ds(col, LANES)], buf.at[pl.ds(u, n), yy, xx]
        else:
            for j in range(n):
                lanes = pl.ds(pl.multiple_of((u + j) * UNIT, UNIT), UNIT)
                yield t.grad.at[:, :, core, :, lanes], buf.at[u + j]

    def load(k, t):
        def act(u, n):
            for src, dst in blocks(t, u, n, c, t.own):
                pltpu.make_async_copy(src, dst, t.ld.at[k]).start()
        t.sized(k, act)

    def exchange(k, t):
        def act(u, n):
            for src, dst in blocks(t, u, n, 1 - c, t.half):
                send(src, dst, t.snd.at[0], t.ra.at[k], partner)
        t.sized(k, act)

    def first_hop(k, t):
        def act(u, n):
            part = pl.ds(u, n)
            arrived(t.own.at[part], t.ld.at[k])
            arrived(t.half.at[part], t.ra.at[k])
            for j in range(n):
                for yy in range(2):
                    t.own[u + j, yy, 1 - x, :HALF] += t.half[u + j, yy, 1 - x, :HALF]
            send(t.own.at[part, :, 1 - x, pl.ds(0, HALF)], t.first_x.at[part], t.snd.at[1], t.rfx.at[k], xnbr)
            for j in range(n):
                for xx in range(2):
                    t.own[u + j, 1 - y, xx, HALF:] += t.half[u + j, 1 - y, xx, HALF:]
            send(t.own.at[part, 1 - y, :, pl.ds(HALF, HALF)], t.first_y.at[part], t.snd.at[2], t.rfy.at[k], ynbr)
        t.sized(k, act)

    def second_hop(k, t):
        def act(u, n):
            part = pl.ds(u, n)
            arrived(t.first_x.at[part], t.rfx.at[k])
            for j in range(n):
                t.own[u + j, 1 - y, x, :HALF] += t.half[u + j, 1 - y, x, :HALF] + t.first_x[u + j, 1 - y]
            send(t.own.at[part, 1 - y, x, pl.ds(0, HALF)], t.second_x.at[part], t.snd.at[3], t.rgx.at[k], ynbr)
            arrived(t.first_y.at[part], t.rfy.at[k])
            for j in range(n):
                t.own[u + j, y, 1 - x, HALF:] += t.half[u + j, y, 1 - x, HALF:] + t.first_y[u + j, 1 - x]
            send(t.own.at[part, y, 1 - x, pl.ds(HALF, HALF)], t.second_y.at[part], t.snd.at[4], t.rgy.at[k], xnbr)
        t.sized(k, act)

    def tile(u):
        return pl.ds(pl.multiple_of(u * UNIT, UNIT), UNIT)

    def finish(k, t):
        def landed(u, n):
            arrived(t.second_x.at[pl.ds(u, n)], t.rgx.at[k])
            arrived(t.second_y.at[pl.ds(u, n)], t.rgy.at[k])

        def one(u):
            first = t.own[u, y, x, :HALF] + t.half[u, y, x, :HALF] + t.first_x[u, y] + t.second_x[u]
            last = t.own[u, y, x, HALF:] + t.half[u, y, x, HALF:] + t.first_y[u, x] + t.second_y[u]
            sq_first = first * first + EPS_ONE
            sq_last = last * last + EPS_ONE
            if t.is_emb:
                t.dirn[pl.ds(pl.multiple_of(u * UNIT, HALF), HALF), :] = first
                t.dirn[pl.ds(pl.multiple_of(u * UNIT + HALF, HALF), HALF), :] = last
                t.col_acc[...] += fold8(sq_first) + fold8(sq_last)
                sq = jnp.transpose(jnp.concatenate([sq_first, sq_last], axis=0))
                t.rpart[0, u] = jnp.sum(fold8(sq), axis=0, keepdims=True)
            else:
                t.dirn[:HALF, tile(u)] = first
                t.dirn[HALF:, tile(u)] = last
                t.col_acc[:HALF] += sq_first
                t.col_acc[HALF:] += sq_last
                t.rpart[0, u] = jnp.sum(fold8(sq_first) + fold8(sq_last), axis=0, keepdims=True)

        def pass_on(u, n):
            send(t.rpart.at[0, pl.ds(u, n)], t.rrecv.at[0, pl.ds(u, n)], t.snd.at[5], t.rr[0].at[k], ring[0])

        def to_all(u, n):
            for o in range(1, nd):
                send(t.rpart.at[0, pl.ds(u, n)], t.rall.at[d, pl.ds(u - hop_units, n)], rall_snd.at[0],
                     rall_sem.at[k - t.hops], (z, lax.rem(d + o, nd)))

        t.sized(k, landed)
        t.units(k, one)
        t.sized(k, pass_on, k < t.hops)
        if not t.is_emb:
            @pl.when(k == t.chunks - 1)
            def _():
                send_cols(t)

            t.sized(k, to_all, k >= t.hops)

    def row_hop(s, k, t):
        def act(u, n):
            part = pl.ds(u, n)
            arrived(t.rrecv.at[s - 1, part], t.rr[s - 1].at[k])
            t.rpart[s, part] = t.rpart[s - 1, part] + t.rrecv[s - 1, part]
            send(t.rpart.at[s, part], t.rrecv.at[s, part], t.snd.at[5 + s], t.rr[s].at[k], ring[s])
        t.sized(k, act, k < t.hops)

    def complete(k, t):
        def landed(u, n):
            part = pl.ds(u, n)
            arrived(t.rrecv.at[2, part], t.rr[2].at[k])
            t.rsum[part] = t.rpart[2, part] + t.rrecv[2, part]

        def landed_all(u, n):
            part = pl.ds(u - hop_units, n)
            arrived(t.rall.at[pl.ds(0, nd - 1), part], rall_sem.at[k - t.hops])
            t.rall[d, part] = t.rpart[0, pl.ds(u, n)]
            t.rsum[pl.ds(u, n)] = jnp.sum(t.rall[:, part], axis=0)

        def one(u):
            row = u if t.is_emb else units + u
            new = BETA_TWO * old[pl.ds(row, 1), :] + (1.0 - BETA_TWO) * (t.rsum[u] / embed)
            t.row_new[pl.ds(u, 1), :] = new
            t.r_acc[...] += new
            line = jnp.broadcast_to(lax.rsqrt(new), (LANES, LANES))
            if t.is_emb:
                n = t.dirn[tile(u), :] * jnp.transpose(line)
                t.dirn[tile(u), :] = n
                t.w_acc[...] += fold8(n * n)
                p = t.pcopy[tile(u), :]
            else:
                n = t.dirn[:, tile(u)] * line
                t.dirn[:, tile(u)] = n
                t.w_acc[...] += n * n
                p = t.pcopy[:, tile(u)]
            t.p_acc[...] += fold8(p * p)

        t.sized(k, landed, k < t.hops)
        if not t.is_emb:
            t.sized(k, landed_all, k >= t.hops)
        t.units(k, one)

    def per_col(t, acc):
        a = acc[...]
        return jnp.sum(a if t.is_emb else jnp.transpose(a), axis=0, keepdims=True)

    def send_cols(t):
        t.vec[0] = per_col(t, t.col_acc)
        for o in range(1, nz):
            send(t.vec.at[0], t.colx.at[z], t.one.at[0], t.one.at[1], (lax.rem(z + o, nz), d))

    def columns(t):
        at = 2 * units + (0 if t.is_emb else 1)
        kept = BETA_TWO * old[at:at + 1, :]
        arrived(t.colx.at[pl.ds(0, nz - 1)], t.one.at[1])
        t.colx[z] = t.vec[0]
        col_sq = t.colx[0]
        for i in range(1, nz):
            col_sq = col_sq + t.colx[i]
        new = kept + (1.0 - BETA_TWO) * (col_sq / vocab)
        t.col_new[...] = new
        inverse = 1.0 / new
        t.scale[...] = inverse if t.is_emb else jnp.transpose(jnp.broadcast_to(inverse, (LANES, LANES)))

    def send_scalars(t):
        w = lane_sum(jnp.sum(fold8(t.w_acc[...] * t.scale[...]), axis=0, keepdims=True))
        r = lane_sum(t.r_acc[...]) / nd
        p = lane_sum(jnp.sum(t.p_acc[...], axis=0, keepdims=True))
        lane = lax.broadcasted_iota(jnp.int32, (1, LANES), 1)
        t.vec[1] = jnp.where(lane == 0, w, jnp.where(lane == 1, r, jnp.where(lane == 2, p, 0.0)))
        for far in range(nz):
            plane = jnp.where(z < nz // 2, nz - 1 - far, far)
            for o in range(1, nd):
                send(t.vec.at[1], t.scalx.at[me], t.one.at[2], t.one.at[3], (plane, lax.rem(d + o, nd)))

            @pl.when(plane != z)
            def _():
                send(t.vec.at[1], t.scalx.at[me], t.one.at[2], t.one.at[3], (plane, d))

    def finish_scalars(t):
        line = lax.rsqrt(t.col_new[...])
        if t.is_emb:
            t.scale[...] = line
        else:
            t.scale[...] = jnp.transpose(jnp.broadcast_to(line, (LANES, LANES)))
        arrived(t.scalx.at[pl.ds(0, others)], t.one.at[3])
        t.scalx[me] = t.vec[1]
        total = jnp.sum(t.scalx[...], axis=0)
        lane = lax.broadcasted_iota(jnp.int32, (1, LANES), 1)
        w, r, p = (lane_sum(jnp.where(lane == i, total, 0.0)) for i in range(3))
        row_mean = r / vocab
        update_rms = jnp.sqrt(w * row_mean / (vocab * embed))
        param_rms = jnp.sqrt(p / (vocab * embed))
        step_size = LEARN_RATE * jnp.maximum(SCALE_FLOOR, param_rms) / jnp.maximum(1.0, update_rms / CLIP_LIMIT)
        t.scale[...] = t.scale[...] * (jnp.sqrt(row_mean) * step_size)

    def update_emb():
        def one(u, carry):
            new = emb.pcopy[tile(u), :] - emb.dirn[tile(u), :] * emb.scale[...]
            emb.dirn[tile(u), :] = new
            emb.b16[tile(u), :] = new.astype(jnp.bfloat16)
            return carry

        lax.fori_loop(0, units, one, 0)

    barrier = pltpu.get_barrier_semaphore()
    above, below = (lax.rem(z + 1, nz), d), (lax.rem(z + nz - 1, nz), d)

    def greet(to):
        pl.semaphore_signal(barrier, inc=1, device_id=to, device_id_type=MESH)

    for peer in ring:
        greet(peer)

    @pl.when(z < nz - 1)
    def _():
        greet(above)

    @pl.when(z > 0)
    def _():
        greet(below)

    for k in range(AHEAD):
        load(k, emb)
    for t in (emb, head):
        for acc in (t.col_acc, t.w_acc, t.r_acc, t.p_acc):
            acc[...] = jnp.zeros_like(acc)
    pl.semaphore_wait(barrier, 3 + jnp.where(z < nz - 1, 1, 0) + jnp.where(z > 0, 1, 0))

    for k in range(AHEAD):
        exchange(k, emb)

    def both(k, act):
        @pl.when((k >= 0) & (k < chunks))
        def _():
            act(k, emb)

        @pl.when((k >= chunks) & (k < total))
        def _():
            act(k - chunks, head)

    def fetch(k, t):
        load(k, t)
        exchange(k, t)

    def relay(r):
        for turn, source, last, to, sem in ((z, 0, nz - 1, above, token.at[0]), (nz - 1 - z, nz - 1, 0, below, token.at[1])):
            @pl.when(r == turn)
            def _():
                @pl.when(z != source)
                def _():
                    pl.semaphore_wait(sem, 1)

                @pl.when(z != last)
                def _():
                    pl.semaphore_signal(sem, inc=1, device_id=to, device_id_type=MESH)

    known = max(chunks - 1 + LAGS[1], LAGS[4] + 1 + nz)

    def step(i, carry):
        both(i + AHEAD, fetch)
        both(i, first_hop)

        @pl.when(i == PSTART)
        def _():
            for t in (emb, head):
                pltpu.make_async_copy(t.param, t.pcopy, t.one.at[4]).start()
            for i, (first, n) in enumerate(old_rows):
                pltpu.make_async_copy(old_in[i], old.at[pl.ds(first, n)], old_sem.at[i]).start()

        both(i - LAGS[0], second_hop)

        @pl.when(i == LAGS[4] - 1)
        def _():
            for t in (emb, head):
                arrived(t.pcopy, t.one.at[4])
            for i, (first, n) in enumerate(old_rows):
                arrived(old.at[pl.ds(first, n)], old_sem.at[i])

        both(i - LAGS[1], finish)
        relay(i - LAGS[4] - 1)

        @pl.when(i == known)
        def _():
            send_cols(emb)

        both(i - LAGS[2], functools.partial(row_hop, 1))
        both(i - LAGS[3], functools.partial(row_hop, 2))

        @pl.when(i == total - 1 + LAGS[4])
        def _():
            columns(head)

        both(i - LAGS[4], complete)

        @pl.when(i == total + 2)
        def _():
            columns(emb)
            send_scalars(emb)

        return carry

    lax.fori_loop(0, total + LAGS[4], step, 0)
    send_scalars(head)
    finish_scalars(emb)
    update_emb()
    finish_scalars(head)

    for t in (emb, head):
        arrived(t.half, t.snd.at[0])
        arrived(t.first_x, t.snd.at[1])
        arrived(t.first_y, t.snd.at[2])
        arrived(t.second_x, t.snd.at[3])
        arrived(t.second_y, t.snd.at[4])
        hopped = t.rpart if t.is_emb else t.rpart.at[:, pl.ds(0, hop_units)]
        for s in range(3):
            arrived(hopped.at[s], t.snd.at[5 + s])
        arrived(t.colx.at[pl.ds(0, nz - 1)], t.one.at[0])
        arrived(t.scalx.at[pl.ds(0, others)], t.one.at[2])
    arrived(head.rall.at[pl.ds(0, nd - 1)], rall_snd.at[0])


def statistics(mesh, emb_grad, head_grad, emb_param, head_param, emb_row, emb_col, head_row, head_col):
    rows, embed = emb_grad.shape
    units = rows // UNIT
    chunks = max(s + (units - s) // BIG for s in (EMB_SMALLS, HEAD_SMALLS))
    nz, nd = mesh.shape["model"], mesh.shape["data"]
    f32 = jnp.float32
    old = [pltpu.with_memory_space_constraint(a.reshape(a.shape[0] // LANES, LANES), pltpu.HBM)
           for a in (emb_row, head_row, emb_col, head_col)]

    buffers = [pltpu.VMEM((units, 2, 2, UNIT, LANES), f32), pltpu.VMEM((units, 2, 2, UNIT, LANES), f32),
               pltpu.VMEM((units, 2, HALF, LANES), f32), pltpu.VMEM((units, 2, HALF, LANES), f32),
               pltpu.VMEM((units, HALF, LANES), f32), pltpu.VMEM((units, HALF, LANES), f32)]

    def small(acc_rows):
        return [pltpu.VMEM((3, units, 1, LANES), f32), pltpu.VMEM((3, units, 1, LANES), f32),
                pltpu.VMEM((units, 1, LANES), f32), pltpu.VMEM((nd, min(DIRECT, HEAD_SMALLS) + max(DIRECT - HEAD_SMALLS, 0) * BIG, 1, LANES), f32),
                pltpu.VMEM((acc_rows, LANES), f32), pltpu.VMEM((acc_rows, LANES), f32),
                pltpu.VMEM((1, LANES), f32), pltpu.VMEM((8, LANES), f32),
                pltpu.VMEM((nz, 1, LANES), f32), pltpu.VMEM((nz * nd, 1, LANES), f32), pltpu.VMEM((2, 1, LANES), f32)]

    sems = [pltpu.SemaphoreType.DMA((chunks,)) for _ in range(9)]
    sems += [pltpu.SemaphoreType.DMA((8,)), pltpu.SemaphoreType.DMA((5,))]

    stats = [jax.ShapeDtypeStruct((units, LANES), f32), jax.ShapeDtypeStruct((1, LANES), f32)]
    emb_outs = [jax.ShapeDtypeStruct((rows, LANES), f32), jax.ShapeDtypeStruct((rows, LANES), jnp.bfloat16)] + stats
    head_outs = [jax.ShapeDtypeStruct((LANES, rows), f32)] * 2 + stats + [jax.ShapeDtypeStruct((LANES, LANES), f32)]
    hbm = pl.BlockSpec(memory_space=pltpu.HBM)
    vmem = pl.BlockSpec(memory_space=pltpu.VMEM)
    results = pl.pallas_call(
        functools.partial(adafactor_kernel, units, nz, nd),
        out_shape=emb_outs + head_outs,
        in_specs=[hbm] * 8,
        out_specs=[vmem] * 9,
        scratch_shapes=(buffers + buffers + small(8) + small(LANES) + sems + sems
                        + [pltpu.SemaphoreType.REGULAR((2,)), pltpu.SemaphoreType.DMA((DIRECT,)),
                           pltpu.SemaphoreType.DMA((1,)), pltpu.VMEM((2 * units + 2, LANES), f32),
                           pltpu.SemaphoreType.DMA((4,)), pltpu.VMEM((rows, LANES), f32), pltpu.VMEM((1, LANES), f32)]),
        compiler_params=pltpu.CompilerParams(collective_id=0, has_side_effects=True, vmem_limit_bytes=VMEM_KIB * 1024),
    )(emb_grad.reshape(units, UNIT, embed), emb_param, head_grad.reshape(2, 2, 2, LANES, rows), head_param, *old)
    return results


PIECES = 8


def apply_kernel(rows, *refs):
    ready, (head_dir, head_p, head_r, head_c, head_s) = refs[:4], refs[4:9]
    out, (head_new, head_b16, head_ro, head_co) = refs[9:13], refs[13:17]
    head_tmp, head_tmp16, sem = refs[17:]
    for i, (src, dst) in enumerate(zip(ready + (head_r, head_c), out + (head_ro, head_co))):
        pltpu.make_async_copy(src, dst, sem.at[2 + i]).start()
    size = rows // PIECES

    def piece(j, carry):
        span = pl.ds(pl.multiple_of(j * size, size), size)
        for i in range(size // LANES):
            cols = pl.ds(pl.multiple_of(j * size + i * LANES, LANES), LANES)
            new = head_p[:, cols] - head_dir[:, cols] * head_s[...]
            head_tmp[:, cols] = new
            head_tmp16[:, cols] = new.astype(jnp.bfloat16)
        pltpu.make_async_copy(head_tmp.at[:, span], head_new.at[:, span], sem.at[0]).start()
        pltpu.make_async_copy(head_tmp16.at[:, span], head_b16.at[:, span], sem.at[1]).start()
        return carry

    lax.fori_loop(0, PIECES, piece, 0)
    arrived(head_new, sem.at[0])
    arrived(head_b16, sem.at[1])
    for i, dst in enumerate(out + (head_ro, head_co)):
        arrived(dst, sem.at[2 + i])


def apply_update(results):
    rows = results[0].shape[0]
    f32, b16 = jnp.float32, jnp.bfloat16
    hbm = pl.BlockSpec(memory_space=pltpu.HBM)
    vmem = pl.BlockSpec(memory_space=pltpu.VMEM)
    stats = ((rows // LANES, LANES), f32), ((1, LANES), f32)
    shapes = (((rows, LANES), f32), ((rows, LANES), b16)) + stats + (((LANES, rows), f32), ((LANES, rows), b16)) + stats
    emb_new, emb_b16, emb_r, emb_c, head_new, head_b16, head_r, head_c = pl.pallas_call(
        functools.partial(apply_kernel, rows),
        out_shape=[jax.ShapeDtypeStruct(s, t) for s, t in shapes],
        in_specs=[vmem] * 9,
        out_specs=[hbm] * 8,
        scratch_shapes=[pltpu.VMEM((LANES, rows), f32), pltpu.VMEM((LANES, rows), b16), pltpu.SemaphoreType.DMA((8,))],
        compiler_params=pltpu.CompilerParams(vmem_limit_bytes=24 * 2 ** 20),
    )(*results)
    return (emb_new, head_new, emb_r.reshape(rows), emb_c.reshape(LANES), head_r.reshape(rows), head_c.reshape(LANES),
            emb_b16, head_b16)


def solution(mesh):
    arg_specs = (P("model", "data"), P("data", "model"), P("data", "model", None), P("data", None, "model"),
                 P("model"), P("data"), P("model"), P("data"))
    result_specs = (P("model", "data"), P("data", "model"), P("model"), P("data"), P("model"), P("data"),
                    P("model", "data"), P("data", "model"))

    def local_step(emb_block, head_block, emb_contrib, head_contrib, emb_rows, emb_cols, head_rows, head_cols):
        return apply_update(statistics(mesh, emb_contrib[0], head_contrib[0], emb_block, head_block,
                                       emb_rows, emb_cols, head_rows, head_cols))

    return jax.shard_map(local_step, mesh=mesh, in_specs=arg_specs, out_specs=result_specs, check_vma=False)
```
